32 devices in a mesh: gx: 2 (over y), gy: 4 (over x, core), gz: 4 (over z).
Axes of the slice: x: 2, y: 2, z: 4, core: 2. Of those that a mesh axis runs over, the one named last changes fastest.
Arguments:
- halo_position: float32 [3, 16, 16, 8, 128], P(None, 'gx', 'gy', 'gz'), may hold values from 0 to 1
- halo_velocity: float32 [3, 16, 16, 8, 128], P(None, 'gx', 'gy', 'gz'), may hold values from -1 to 1
- halo_mass: float32 [16, 16, 8, 128], P('gx', 'gy', 'gz'), may hold values from 0.005 to 0.08
- cell_counts: int32 [16, 16, 8], P('gx', 'gy', 'gz'), may hold values from 1 to 128, as said below
Outputs:
- predicted: float32 [3, 16, 16, 8, 128], P(None, 'gx', 'gy', 'gz')
The draws below stay inside these ranges and needn't reach their ends.
Inputs may be any that keep to these rules, and one draw needn't show every extreme that they name: `cell_counts`: slots of a cell from its count on hold no halo.
All inputs are finite; a program needn't handle non-finite values.
Results may differ from the reference program's by a relative error of at most 0.0001.
Values sent between devices are 32-bit elements; how exact they have to be, the bound alone decides.
No kernel may reach another device: no remote copies, remote signals or barrier semaphores. Data moves between devices by JAX's collectives and lax.ppermute only.
A program may use at most 64 MiB of HBM per device.

```python
import math
import jax
import jax.numpy as jnp
from jax import lax

CX = 8
CY = 4
CZ = 2
SLOTS = 128
NX = 16
NY = 16
NZ = 8


def draw_cell_counts(key, part):
    key_level, key_fill, key_peak = jax.random.split(key, 3)
    levels = jax.random.randint(key_level, (NX // CX, NY // CY, NZ // CZ), 0, 4)
    factor = jnp.left_shift(jnp.ones_like(levels), levels)
    factor = jnp.repeat(jnp.repeat(jnp.repeat(factor, CX, axis=0), CY, axis=1), CZ, axis=2)
    filled = jax.random.randint(key_fill, (NX, NY, NZ), 0, max(SLOTS // 4, 1))
    counts = jnp.minimum(1 + factor * filled, SLOTS)
    peak_cell = jax.random.randint(key_peak, (), 0, NX * NY * NZ)
    flattened = jnp.where(jnp.arange(NX * NY * NZ) == peak_cell, SLOTS, counts.reshape(-1))
    return flattened.reshape(NX, NY, NZ).astype(jnp.int32)


def steps_of(key, dims, cuts, least, top_value):
    def one(position, blocks):
        heights = jax.random.uniform(jax.random.fold_in(jax.random.fold_in(key, 6), position), (blocks,), jnp.float32, least / len(cuts), top_value / len(cuts))
        return jnp.repeat(jnp.exp(heights), dims[position] // blocks).reshape((-1,) + (1,) * (len(dims) - position - 1))

    loudness = one(*cuts[0])
    for cut in cuts[1:]:
        loudness = loudness * one(*cut)
    return loudness


def scatter_about(rng, extent, width, limit, cuts=(), kind=jnp.bfloat16):
    entries = width * jax.random.normal(rng, extent, jnp.float32)
    if cuts:
        entries = entries * steps_of(rng, extent, cuts, -0.22, 0.18)
    return jnp.clip(entries, -limit, limit).astype(kind)


def setup_inputs(seed: int = 0) -> dict:
    key_of = jax.random.split(jax.random.key(seed), 5)
    halo_position = jnp.clip(1.0 * jax.random.uniform(key_of[0], (3, NX, NY, NZ, SLOTS), jnp.float32) ** steps_of(key_of[0], (3, NX, NY, NZ, SLOTS), ((1, 2), (2, 4), (3, 4)), -0.2, 0.2), 0.0, 1.0)
    halo_velocity = scatter_about(key_of[1], (3, NX, NY, NZ, SLOTS), 0.2, 1.0, ((1, 2), (2, 4), (3, 4)), jnp.float32)
    halo_mass = jnp.clip(jnp.exp(math.log(0.08) - 2.7725887 * jax.random.uniform(key_of[2], (NX, NY, NZ, SLOTS), jnp.float32) ** steps_of(key_of[2], (NX, NY, NZ, SLOTS), ((0, 2), (1, 4), (2, 4)), -0.2, 0.2)), 0.005, 0.08)
    cell_counts = draw_cell_counts(jax.random.fold_in(key_of[4], 71), 0)
    return dict(halo_position=halo_position, halo_velocity=halo_velocity, halo_mass=halo_mass, cell_counts=cell_counts)


soft_sq = 0.01
cut_sq = 0.64

def pull_block(extended, targets):
    depth_x, depth_y, depth_z, slot_count = targets.shape[1:]
    anchor = jnp.int32(0)

    def add_offset(offset_code, running):
        offset_code = offset_code.astype(jnp.int32)
        shift_x = offset_code // 9
        shift_y = offset_code // 3 % 3
        shift_z = offset_code % 3
        sources = lax.dynamic_slice(extended, (anchor, shift_x, shift_y, shift_z, anchor), (4, depth_x, depth_y, depth_z, slot_count))
        delta_x = (sources[0] + (shift_x - 1).astype(jnp.float32))[..., :, None] - targets[0][..., None, :]
        delta_y = (sources[1] + (shift_y - 1).astype(jnp.float32))[..., :, None] - targets[1][..., None, :]
        delta_z = (sources[2] + (shift_z - 1).astype(jnp.float32))[..., :, None] - targets[2][..., None, :]
        dist_sq = delta_x * delta_x + delta_y * delta_y + delta_z * delta_z
        inv_dist = lax.rsqrt(dist_sq + soft_sq)
        tapering = jnp.maximum(1.0 - dist_sq / cut_sq, 0.0)
        weights = sources[3][..., :, None] * (inv_dist * inv_dist * inv_dist) * (tapering * tapering)
        return running + jnp.stack([lax.optimization_barrier(jnp.sum(weights * delta_x, axis=-2)), lax.optimization_barrier(jnp.sum(weights * delta_y, axis=-2)), lax.optimization_barrier(jnp.sum(weights * delta_z, axis=-2))], axis=0)
    return lax.fori_loop(jnp.int32(0), jnp.int32(27), add_offset, jnp.zeros(targets.shape, jnp.float32))

def pull_grid(field):
    padded = jnp.pad(field, ((0, 0), (1, 1), (1, 1), (1, 1), (0, 0)), mode='wrap')

    def one_plane(plane_index):
        window = lax.dynamic_slice_in_dim(padded, plane_index, 3, axis=1)
        targets = lax.dynamic_slice_in_dim(field[:3], plane_index, 1, axis=1)
        return pull_block(window, targets)[:, 0]
    planes = lax.map(one_plane, jnp.arange(field.shape[1], dtype=jnp.int32))
    return jnp.moveaxis(planes, 0, 1)

def reference(halo_position, halo_velocity, halo_mass, cell_counts):
    occupied = lax.broadcasted_iota(jnp.int32, halo_mass.shape, 3) < cell_counts[..., None]
    held_mass = jnp.where(occupied, halo_mass, 0.0)
    first_pull = pull_grid(jnp.concatenate([halo_position, held_mass[None]], axis=0))
    drifted = halo_position + halo_velocity + 0.5 * first_pull
    second_pull = pull_grid(jnp.concatenate([drifted, held_mass[None]], axis=0))
    predicted = halo_position + halo_velocity + first_pull / 3.0 + second_pull / 6.0
    return jnp.where(occupied[None], predicted, 0.0)
```

```python
import functools
import jax, jax.numpy as jnp
from jax import lax
from jax.sharding import PartitionSpec as P
from jax.experimental import pallas as pl
from jax.experimental.pallas import tpu as pltpu

soft_sq = 0.01
cut_sq = 0.64
f32, bf16 = jnp.float32, jnp.bfloat16


def rounded(v):
    return v.astype(bf16).astype(f32)


def split3(v):
    a = rounded(v)
    rest = v - a
    b = rounded(rest)
    return a, b, rest - b


def squares(v, extra=0.0):
    a = rounded(v)
    rest = v - a
    b = rounded(rest)
    top = a * a
    top_a = rounded(top)
    low = 2.0 * a * rest + rest * rest + extra
    la, lb, lc = split3(low)
    return (a, b, rest - b), (top_a, top - top_a, la, lb, lc)


def source_rows(v):
    (a, b, c), (pa, pb, pc, pd, pe) = squares(v)
    one = jnp.ones_like(v)
    return [a, one, one, pa, pb, a, b, b, a, c, one, one, one, pc, pd, pe]


def target_rows(v, extra):
    (a, b, c), (pa, pb, pc, pd, pe) = squares(v, extra)
    one = jnp.ones_like(v)
    return [-2.0 * a, pa, pb, one, one, -2.0 * b, -2.0 * a, -2.0 * b, -2.0 * c, -2.0 * a, pc, pd, pe, one, one, one]


def pull_kernel(grid, ext_ref, own_ref, out_ref, left, sums, right, rows):
    nx, ny, nz = grid
    ey, ez = ny + 2, nz + 2
    cells = ext_ref.shape[1]
    own = own_ref.shape[1]

    def prep_sources(i, _):
        at = pl.ds(pl.multiple_of(i * 8, 8), 8)
        where = 0
        for d in range(3):
            for piece in source_rows(ext_ref[d, at, :] - 0.5):
                rows[where * 8:where * 8 + 8, :] = piece
                where += 1
        mass = ext_ref[3, at, :] * (1.0 / (cut_sq * cut_sq))
        pieces = list(split3(mass))
        for d in range(3):
            pieces += list(split3(mass * (ext_ref[d, at, :] - 0.5)))
        for piece in pieces:
            rows[where * 8:where * 8 + 8, :] = piece
            where += 1
        for j in range(8):
            block = rows[pl.ds(j, 48, stride=8), :]
            left[i * 8 + j] = block.T.astype(bf16)
            block = rows[pl.ds(48 * 8 + j, 16, stride=8), :]
            sums[i * 8 + j] = block.astype(bf16)
        return 0

    rows[...] = jnp.zeros_like(rows)
    lax.fori_loop(0, cells // 8, prep_sources, 0)

    def prep_targets(i, _):
        at = pl.ds(pl.multiple_of(i * 8, 8), 8)
        for d in range(3):
            base = own_ref[d, at, :] - 0.5
            for o in range(3):
                for k, piece in enumerate(target_rows(base - float(o - 1), soft_sq if d == 2 else 0.0)):
                    rows[k * 8:k * 8 + 8, :] = piece
                for j in range(8):
                    block = rows[pl.ds(j, 16, stride=8), :]
                    right[i * 8 + j, d * 3 + o] = block.astype(bf16)
        return 0

    lax.fori_loop(0, own // 8, prep_targets, 0)

    def one_pair(p, _):
        tx = p // ny
        ty = p % ny
        for z0 in range(0, nz, 2):
            me = p * nz + z0
            acc = jnp.zeros((16, 256), f32)
            side = [jnp.zeros((8, 256), f32) for _ in range(3)]
            for ox in range(3):
                acc_x = jnp.zeros((16, 256), f32)
                for oy in range(3):
                    acc_y = jnp.zeros((16, 256), f32)
                    first = ((tx + ox) * ey + ty + oy) * ez + z0
                    both = [[jnp.concatenate([right[me + t, ox], right[me + t, 3 + oy], right[me + t, 6 + oz]], axis=0)
                             for oz in range(3)] for t in range(2)]
                    for layer in range(4):
                        part = []
                        if layer == 0:
                            rhs = both[0][0]
                        elif layer == 3:
                            rhs = both[1][2]
                        else:
                            rhs = jnp.concatenate([both[0][layer], both[1][layer - 1]], axis=1)
                        q = jnp.dot(left[first + layer], rhs, preferred_element_type=f32)
                        r = lax.rsqrt(q)
                        t = jnp.maximum((cut_sq + soft_sq) - q, 0.0)
                        t = r * t
                        w = t * t * r
                        hi = w.astype(bf16)
                        lo = (w - hi.astype(f32)).astype(bf16)
                        fe = sums[first + layer]
                        got = jnp.dot(jnp.concatenate([fe, fe], axis=1), jnp.concatenate([hi, lo], axis=0), preferred_element_type=f32)
                        if layer == 0:
                            got = jnp.concatenate([got, jnp.zeros_like(got)], axis=1)
                            zed = jnp.concatenate([-got[:8, :128], jnp.zeros((8, 128), f32)], axis=1)
                        elif layer == 3:
                            got = jnp.concatenate([jnp.zeros_like(got), got], axis=1)
                            zed = got[:8]
                        elif layer == 1:
                            zed = jnp.concatenate([jnp.zeros((8, 128), f32), -got[:8, 128:]], axis=1)
                        else:
                            zed = jnp.concatenate([got[:8, :128], jnp.zeros((8, 128), f32)], axis=1)
                        side[2] = side[2] + zed
                        acc_y = acc_y + got
                    if oy != 1:
                        side[1] = side[1] + float(oy - 1) * acc_y[:8]
                    acc_x = acc_x + acc_y
                if ox != 1:
                    side[0] = side[0] + float(ox - 1) * acc_x[:8]
                acc = acc + acc_x
            total = acc[0:1] + acc[1:2] + acc[2:3]
            for d in range(3):
                moment = acc[3 * d + 3:3 * d + 4] + acc[3 * d + 4:3 * d + 5] + acc[3 * d + 5:3 * d + 6]
                shift = side[d][0:1] + side[d][1:2] + side[d][2:3]
                for t in range(2):
                    lanes = slice(128 * t, 128 * t + 128)
                    at = own_ref[d, pl.ds(me + t, 1), :] - 0.5
                    out_ref[d, pl.ds(me + t, 1), :] = (moment[:, lanes] + shift[:, lanes]) - at * total[:, lanes]
        return 0

    lax.fori_loop(0, nx * ny, one_pair, 0)


def pull(ext, own, grid):
    cells = ext.shape[1]
    count = own.shape[1]
    return pl.pallas_call(
        functools.partial(pull_kernel, grid),
        out_shape=jax.ShapeDtypeStruct((3, count, 128), f32),
        in_specs=[pl.BlockSpec(memory_space=pltpu.VMEM)] * 2,
        out_specs=pl.BlockSpec(memory_space=pltpu.VMEM),
        scratch_shapes=[
            pltpu.VMEM((cells, 128, 48), bf16),
            pltpu.VMEM((cells, 16, 128), bf16),
            pltpu.VMEM((count, 9, 16, 128), bf16),
            pltpu.VMEM((64 * 8, 128), f32),
        ],
        compiler_params=pltpu.CompilerParams(vmem_limit_bytes=60 * 2**20),
    )(ext, own)


def extended_2(cells, sides, width):
    for axis, dim in sides:
        count = lax.axis_size(axis)
        head = lax.slice_in_dim(cells, 0, width, axis=dim)
        tail = lax.slice_in_dim(cells, cells.shape[dim] - width, cells.shape[dim], axis=dim)
        cells = jnp.concatenate(
            [
                lax.ppermute(tail, axis, [(i, (i + 1) % count) for i in range(count)]),
                cells,
                lax.ppermute(head, axis, [((i + 1) % count, i) for i in range(count)]),
            ],
            axis=dim,
        )
    return cells


def pull_field(extended, targets):
    slots = targets.shape[-1]
    flat = pull(extended.reshape(4, -1, slots), targets.reshape(3, -1, slots), targets.shape[1:4])
    return flat.reshape(targets.shape)


def body(halo_position, halo_velocity, halo_mass, cell_counts):
    occupied = lax.broadcasted_iota(jnp.int32, halo_mass.shape, 3) < cell_counts[..., None]
    held_mass = jnp.where(occupied, halo_mass, 0.0)
    outgoing = jnp.concatenate([halo_position, held_mass[None]], axis=0)
    mass_rim = None
    first_pull = None
    second_pull = None
    for round_index in range(2):
        widened = extended_2(outgoing, (("gx", 1),), 1)
        widened = extended_2(widened, (("gy", 2),), 1)
        widened = extended_2(widened, (("gz", 3),), 1)
        if round_index == 0:
            mass_rim = widened[3:4]
            first_pull = pull_field(widened, halo_position)
            outgoing = halo_position + halo_velocity + 0.5 * first_pull
        else:
            second_pull = pull_field(jnp.concatenate([widened, mass_rim], axis=0), outgoing)
    predicted = halo_position + halo_velocity + first_pull / 3.0 + second_pull / 6.0
    return jnp.where(occupied[None], predicted, 0.0)


def solution(mesh):
    return jax.shard_map(
        body,
        mesh=mesh,
        in_specs=(
            P(None, "gx", "gy", "gz", None),
            P(None, "gx", "gy", "gz", None),
            P("gx", "gy", "gz", None),
            P("gx", "gy", "gz"),
        ),
        out_specs=P(None, "gx", "gy", "gz", None),
        check_vma=False,
    )
```

```python
import functools
import jax
import jax.numpy as jnp
import numpy as np
from jax import lax
from jax.experimental import pallas as pl
from jax.experimental.pallas import tpu as pltpu
from jax.sharding import PartitionSpec as P

soft_sq = 0.01
cut_sq = 0.64
near = 6.0
f32, bf16 = jnp.float32, jnp.bfloat16


def rounded(v):
    return v.astype(bf16).astype(f32)


def split3(v):
    a = rounded(v)
    rest = v - a
    b = rounded(rest)
    return a, b, rest - b


def squares(v, extra=0.0):
    a = rounded(v)
    rest = v - a
    b = rounded(rest)
    top = a * a
    top_a = rounded(top)
    low = 2.0 * a * rest + rest * rest + extra
    return (a, b, rest - b), (top_a, top - top_a, *split3(low))


def source_rows(v):
    (a, b, c), (pa, pb, pc, pd, pe) = squares(v)
    one = jnp.ones_like(v)
    return [a, one, one, pa, pb, a, b, b, a, c, one, one, one, pc, pd, pe]


def target_rows(v, extra):
    (a, b, c), (pa, pb, pc, pd, pe) = squares(v, extra)
    one = jnp.ones_like(v)
    return [-2.0 * a, pa, pb, one, one, -2.0 * b, -2.0 * a, -2.0 * b, -2.0 * c, -2.0 * a, pc, pd, pe, one, one, one]


def stage_sources(ref, i, rows, base):
    at = pl.ds(pl.multiple_of(i * 8, 8), 8)
    pieces = []
    mass = ref[3, at, :] * (1.0 / (cut_sq * cut_sq))
    sums = list(split3(mass))
    for d in range(3):
        place = ref[d, at, :] - 0.5
        pieces += source_rows(place)
        sums += list(split3(mass * place))
    for k, piece in enumerate(pieces + sums):
        rows[base + k * 8:base + k * 8 + 8, :] = piece


def staged(rows, base, j, first, count):
    return rows[pl.ds(base + first * 8 + j, count, stride=8), :]


def stage_targets(own_ref, rows, right):
    def some(i, _):
        at = pl.ds(pl.multiple_of(i * 8, 8), 8)
        for d in range(3):
            base = own_ref[d, at, :] - 0.5
            for o in range(3):
                for k, piece in enumerate(target_rows(base - float(o - 1), soft_sq if d == 2 else 0.0)):
                    rows[k * 8:k * 8 + 8, :] = piece
                for j in range(8):
                    right[i * 8 + j, d * 3 + o] = staged(rows, 0, j, 0, 16).astype(bf16)
        return 0

    lax.fori_loop(0, own_ref.shape[1] // 8, some, 0)


def weighted(left, right, moments):
    q = jnp.dot(left, right, preferred_element_type=f32)
    r = lax.rsqrt(q)
    t = jnp.maximum((cut_sq + soft_sq) - q, 0.0) * r
    w = t * t * r
    hi = w.astype(bf16)
    lo = (w - hi.astype(f32)).astype(bf16)
    return jnp.dot(
        jnp.concatenate([moments, moments], axis=1), jnp.concatenate([hi, lo], axis=0), preferred_element_type=f32
    )


def pull_kernel(plan, *refs):
    kind, group, has_before = plan
    items = refs[0]
    own_ref = refs[1]
    sources = {"own": 1, "caps": 2, "rim": 4}[kind]
    source_refs = refs[1:2] if kind == "own" else refs[2:2 + sources]
    at = 2 if kind == "own" else 2 + sources
    before = refs[at] if has_before else None
    at += int(has_before)
    out_ref, right, rows, acc, raw, *feats = refs[at:]
    columns = own_ref.shape[1] // 2
    count = items.shape[0] // 4

    widest = jnp.zeros((), f32)
    for ref in (own_ref, *(source_refs if kind != "own" else ())):
        widest = jnp.maximum(widest, jnp.max(jnp.abs(ref[0:3] - 0.5)))
    calm = widest < near

    def read(n):
        return items[4 * n], items[4 * n + 1], items[4 * n + 2], items[4 * n + 3]

    @pl.when(calm)
    def _():
        acc[...] = jnp.zeros_like(acc)
        if kind == "own":
            left, sums = feats

            def some(i, _):
                stage_sources(own_ref, i, rows, 0)
                for j in range(8):
                    left[i * 8 + j] = staged(rows, 0, j, 0, 48).T.astype(bf16)
                    sums[i * 8 + j] = staged(rows, 0, j, 48, 16).astype(bf16)
                return 0

            lax.fori_loop(0, own_ref.shape[1] // 8, some, 0)
        elif kind == "caps":
            left_caps, sums_caps = feats

            def some(i, _):
                for side in range(2):
                    stage_sources(source_refs[side], i, rows, side * 512)
                for j in range(8):
                    both = [staged(rows, side * 512, j, 0, 48) for side in range(2)]
                    left_caps[i * 8 + j] = jnp.concatenate(both, axis=0).T.astype(bf16)
                    both = [staged(rows, side * 512, j, 48, 16) for side in range(2)]
                    sums_caps[i * 8 + j] = jnp.concatenate(both, axis=0).astype(bf16)
                return 0

            lax.fori_loop(0, source_refs[0].shape[1] // 8, some, 0)
        else:
            left, sums, left_caps, sums_caps = feats
            base = 0
            for ref in source_refs:

                def some(i, _, ref=ref, base=base):
                    stage_sources(ref, i, rows, 0)
                    for c in range(2):
                        column = base + i * 2 + c
                        for z in range(2):
                            left[column * 2 + z] = staged(rows, 0, 4 * c + 1 + z, 0, 48).T.astype(bf16)
                            sums[column * 2 + z] = staged(rows, 0, 4 * c + 1 + z, 48, 16).astype(bf16)
                        both = [staged(rows, 0, 4 * c + 3 * side, 0, 48) for side in range(2)]
                        left_caps[column] = jnp.concatenate(both, axis=0).T.astype(bf16)
                        both = [staged(rows, 0, 4 * c + 3 * side, 48, 16) for side in range(2)]
                        sums_caps[column] = jnp.concatenate(both, axis=0).astype(bf16)
                    return 0

                lax.fori_loop(0, ref.shape[1] // 8, some, 0)
                base += ref.shape[1] // 4
        stage_targets(own_ref, rows, right)

        def some_items(g, _):
            for k in range(group):
                column, source, ox, oy = read(g * group + k)
                me = jnp.minimum(column, columns - 1) * 2
                side = [[jnp.concatenate([right[me + t, ox], right[me + t, 3 + oy], right[me + t, 6 + oz]], axis=0)
                         for oz in range(3)] for t in range(2)]
                got = None
                zed = None
                if kind != "caps":
                    low = weighted(left[source * 2], jnp.concatenate([side[0][1], side[1][0]], axis=1), sums[source * 2])
                    high = weighted(left[source * 2 + 1], jnp.concatenate([side[0][2], side[1][1]], axis=1), sums[source * 2 + 1])
                    got = low + high
                    zed = jnp.concatenate([high[:8, :128], -low[:8, 128:]], axis=1)
                if kind != "own":
                    blank = jnp.zeros_like(side[0][0])
                    right_caps = jnp.concatenate(
                        [jnp.concatenate([side[0][0], blank], axis=1), jnp.concatenate([blank, side[1][2]], axis=1)], axis=0
                    )
                    caps = weighted(left_caps[source], right_caps, sums_caps[source])
                    caps_got = jnp.concatenate([caps[:16, :128], caps[16:, 128:]], axis=1)
                    caps_zed = jnp.concatenate([-caps[:8, :128], caps[16:24, 128:]], axis=1)
                    got = caps_got if got is None else got + caps_got
                    zed = caps_zed if zed is None else zed + caps_zed
                head = got[:8]
                for t in range(2):
                    lanes = slice(128 * t, 128 * t + 128)
                    first = pl.multiple_of((t * (columns + 1) + column) * 40, 8)
                    acc[pl.ds(first, 16), :] += got[:, lanes]
                    acc[pl.ds(first + 16, 8), :] += (ox - 1).astype(f32) * head[:, lanes]
                    acc[pl.ds(first + 24, 8), :] += (oy - 1).astype(f32) * head[:, lanes]
                    acc[pl.ds(first + 32, 8), :] += zed[:, lanes]
            return 0

        lax.fori_loop(0, count // group, some_items, 0)

        def finish(i, _):
            for t in range(2):
                def row(r):
                    return acc[pl.ds((t * (columns + 1) + i * 8) * 40 + r, 8, stride=40), :]

                spot = pl.ds(i * 16 + t, 8, stride=2)
                total = row(0) + row(1) + row(2)
                for d in range(3):
                    moment = row(3 * d + 3) + row(3 * d + 4) + row(3 * d + 5)
                    moment = moment + (row(16 + 8 * d) + row(17 + 8 * d) + row(18 + 8 * d))
                    value = moment - (own_ref[d, spot, :] - 0.5) * total
                    if has_before:
                        value = value + before[d, spot, :]
                    out_ref[d, spot, :] = value
            return 0

        lax.fori_loop(0, columns // 8, finish, 0)

    @pl.when(jnp.logical_not(calm))
    def _():
        raw[...] = jnp.zeros_like(raw)
        base = 0
        for ref in source_refs:

            def keep(cell, _, ref=ref, base=base):
                for d in range(4):
                    raw[base + cell, d:d + 1, :] = ref[d, pl.ds(cell, 1), :]
                return 0

            lax.fori_loop(0, ref.shape[1], keep, 0)
            base += ref.shape[1]
        out_ref[...] = before[...] if has_before else jnp.zeros_like(out_ref)
        layers = {"own": (1, 2), "caps": (0, 3), "rim": (0, 1, 2, 3)}[kind]

        def one(n, _):
            column, source, ox, oy = read(n)

            @pl.when(column < columns)
            def _():
                for layer in layers:
                    cell = {"own": source * 2 + layer - 1, "caps": source + (layer // 3) * columns, "rim": source * 4 + layer}[kind]
                    lined = raw[cell].T
                    for t in range(2):
                        if abs(layer - 1 - t) > 1:
                            continue
                        spot = pl.ds(column * 2 + t, 1)
                        offset = ((ox - 1).astype(f32), (oy - 1).astype(f32), float(layer - 1 - t))
                        away = [(lined[:, d:d + 1] + offset[d]) - own_ref[d, spot, :] for d in range(3)]
                        q = away[0] * away[0] + away[1] * away[1] + away[2] * away[2]
                        r = lax.rsqrt(q + soft_sq)
                        taper = jnp.maximum(1.0 - q * (1.0 / cut_sq), 0.0)
                        w = lined[:, 3:4] * (r * r * r) * (taper * taper)
                        for d in range(3):
                            out_ref[d, spot, :] += jnp.sum(w * away[d], axis=0, keepdims=True)
            return 0

        lax.fori_loop(0, count, one, 0)


def listed(grid, kind):
    nx, ny = grid
    found = []
    for tx in range(nx):
        for ty in range(ny):
            for ox in range(3):
                for oy in range(3):
                    x, y = tx + ox - 1, ty + oy - 1
                    inside = 0 <= x < nx and 0 <= y < ny
                    if inside and kind != "rim":
                        found.append((tx * ny + ty, x * ny + y, ox, oy))
                    elif not inside and kind == "rim":
                        if x < 0:
                            source = 2 * nx + y + 1
                        elif x >= nx:
                            source = 2 * nx + ny + 2 + y + 1
                        else:
                            source = x if y < 0 else nx + x
                        found.append((tx * ny + ty, source, ox, oy))
    return found


def pull(kind, grid, group, own, source_arrays, before):
    nx, ny = grid
    columns = nx * ny
    items = listed(grid, kind)
    while len(items) % group:
        items.append((columns, 0, 1, 1))
    table = np.asarray(items, np.int32).reshape(-1)
    cells = sum(a.shape[1] for a in source_arrays) if source_arrays else own.shape[1]
    middle = {"own": cells, "caps": 0, "rim": cells // 2}[kind]
    capped = {"own": 0, "caps": cells // 2, "rim": cells // 4}[kind]
    feats = []
    if middle:
        feats += [pltpu.VMEM((middle, 128, 48), bf16), pltpu.VMEM((middle, 16, 128), bf16)]
    if capped:
        feats += [pltpu.VMEM((capped, 128, 96), bf16), pltpu.VMEM((capped, 32, 128), bf16)]
    args = [own, *source_arrays] + ([before] if before is not None else [])
    pairs = len(items) * (3 if kind == "rim" else 2 if kind == "own" else 1) * 128 * 256
    return pl.pallas_call(
        functools.partial(pull_kernel, (kind, group, before is not None)),
        out_shape=jax.ShapeDtypeStruct((3, own.shape[1], 128), f32),
        in_specs=[pl.BlockSpec(memory_space=pltpu.SMEM)] + [pl.BlockSpec(memory_space=pltpu.VMEM)] * len(args),
        out_specs=pl.BlockSpec(memory_space=pltpu.VMEM),
        scratch_shapes=[
            pltpu.VMEM((own.shape[1], 9, 16, 128), bf16),
            pltpu.VMEM((1024, 128), f32),
            pltpu.VMEM((2 * (columns + 1) * 40, 128), f32),
            pltpu.VMEM((cells, 8, 128), f32),
            *feats,
        ],
        compiler_params=pltpu.CompilerParams(vmem_limit_bytes=40 * 2**20),
        cost_estimate=pl.CostEstimate(flops=pairs * 40, bytes_accessed=2**20, transcendentals=pairs),
        name="pull_" + kind,
    )(jnp.asarray(table), *args)


def passed(axis, tail, head):
    count = lax.axis_size(axis)
    if count == 2:
        both = lax.ppermute(jnp.stack([tail, head]), axis, [(0, 1), (1, 0)])
        return both[0], both[1]
    return (
        lax.ppermute(tail, axis, [(i, (i + 1) % count) for i in range(count)]),
        lax.ppermute(head, axis, [((i + 1) % count, i) for i in range(count)]),
    )


def pull_field(own):
    grid = own.shape[1:3]
    slots = own.shape[-1]

    def lined(cells):
        return cells.reshape(4, -1, slots)

    lower, upper = passed("gz", own[:, :, :, -1:], own[:, :, :, :1])
    total = pull("own", grid, 22, lined(own), [], None)
    lower, upper, total = lax.optimization_barrier((lower, upper, total))
    tall = [
        jnp.concatenate([lower[:, :, row], own[:, :, row], upper[:, :, row]], axis=3)
        for row in (slice(-1, None), slice(0, 1))
    ]
    front, back = passed("gy", *tall)
    total = pull("caps", grid, 55, lined(own), [lined(lower), lined(upper)], total)
    front, back, total = lax.optimization_barrier((front, back, total))
    wide = [
        jnp.concatenate(
            [front[:, row], jnp.concatenate([lower[:, row], own[:, row], upper[:, row]], axis=3), back[:, row]], axis=2
        )
        for row in (slice(-1, None), slice(0, 1))
    ]
    left, right = passed("gx", *wide)
    total = pull("rim", grid, 17, lined(own), [lined(front), lined(back), lined(left), lined(right)], total)
    return total.reshape(3, *own.shape[1:])


def body(halo_position, halo_velocity, halo_mass, cell_counts):
    occupied = lax.broadcasted_iota(jnp.int32, halo_mass.shape, 3) < cell_counts[..., None]
    held_mass = jnp.where(occupied, halo_mass, 0.0)[None]
    first_pull = pull_field(jnp.concatenate([halo_position, held_mass], axis=0))
    drifted = jnp.where(occupied[None], halo_position + halo_velocity + 0.5 * first_pull, 0.0)
    second_pull = pull_field(jnp.concatenate([drifted, held_mass], axis=0))
    predicted = halo_position + halo_velocity + first_pull / 3.0 + second_pull / 6.0
    return jnp.where(occupied[None], predicted, 0.0)


def solution(mesh):
    return jax.shard_map(
        body,
        mesh=mesh,
        in_specs=(
            P(None, "gx", "gy", "gz", None),
            P(None, "gx", "gy", "gz", None),
            P("gx", "gy", "gz", None),
            P("gx", "gy", "gz"),
        ),
        out_specs=P(None, "gx", "gy", "gz", None),
        check_vma=False,
    )
```

```python
import functools
import jax
import jax.numpy as jnp
import numpy as np
from jax import lax
from jax.experimental import pallas as pl
from jax.experimental.pallas import tpu as pltpu
from jax.sharding import PartitionSpec as P

soft_sq = 0.01
cut_sq = 0.64
near = 6.0
f32, bf16 = jnp.float32, jnp.bfloat16


def rounded(v):
    return v.astype(bf16).astype(f32)


def split3(v):
    a = rounded(v)
    rest = v - a
    b = rounded(rest)
    return a, b, rest - b


def squares(v, extra=0.0):
    a = rounded(v)
    rest = v - a
    b = rounded(rest)
    top = a * a
    top_a = rounded(top)
    low = 2.0 * a * rest + rest * rest + extra
    return (a, b, rest - b), (top_a, top - top_a, *split3(low))


def source_rows(v):
    (a, b, c), (pa, pb, pc, pd, pe) = squares(v)
    one = jnp.ones_like(v)
    return [a, one, one, pa, pb, a, b, b, a, c, one, one, one, pc, pd, pe]


def target_rows(v, extra):
    (a, b, c), (pa, pb, pc, pd, pe) = squares(v, extra)
    one = jnp.ones_like(v)
    return [-2.0 * a, pa, pb, one, one, -2.0 * b, -2.0 * a, -2.0 * b, -2.0 * c, -2.0 * a, pc, pd, pe, one, one, one]


def stage_sources(ref, i, rows, base):
    at = pl.ds(pl.multiple_of(i * 8, 8), 8)
    pieces = []
    mass = ref[3, at, :] * (1.0 / (cut_sq * cut_sq))
    sums = list(split3(mass))
    for d in range(3):
        place = ref[d, at, :] - 0.5
        pieces += source_rows(place)
        sums += list(split3(mass * place))
    for k, piece in enumerate(pieces + sums):
        rows[base + k * 8:base + k * 8 + 8, :] = piece


def staged(rows, base, j, first, count):
    return rows[pl.ds(base + first * 8 + j, count, stride=8), :]


def stage_targets(own_ref, rows, right):
    def some(i, _):
        at = pl.ds(pl.multiple_of(i * 8, 8), 8)
        for d in range(3):
            base = own_ref[d, at, :] - 0.5
            for o in range(3):
                for k, piece in enumerate(target_rows(base - float(o - 1), soft_sq if d == 2 else 0.0)):
                    rows[k * 8:k * 8 + 8, :] = piece
                for j in range(8):
                    right[i * 8 + j, d * 3 + o] = staged(rows, 0, j, 0, 16).astype(bf16)
        return 0

    lax.fori_loop(0, own_ref.shape[1] // 8, some, 0)


def weighted(left, right, moments):
    q = jnp.dot(left, right, preferred_element_type=f32)
    r = lax.rsqrt(q)
    t = jnp.maximum((cut_sq + soft_sq) - q, 0.0) * r
    w = t * t * r
    hi = w.astype(bf16)
    lo = (w - hi.astype(f32)).astype(bf16)
    return jnp.dot(
        jnp.concatenate([moments, moments], axis=1), jnp.concatenate([hi, lo], axis=0), preferred_element_type=f32
    )


def pull_kernel(plan, *refs):
    kind, group = plan
    own_ref = refs[1]
    sources = {"own": 0, "caps": 2, "rim": 5}[kind]
    at = 2 + sources
    source_refs = refs[2:at] or refs[1:2]
    before = None
    if kind == "own":
        out_ref, right = refs[at:at + 2]
    else:
        right, before, out_ref = refs[at:at + 3]
        at += 1
    rows, acc, raw, items, copied, *feats = refs[at + 2:]
    fetch = pltpu.make_async_copy(refs[0], items, copied)
    fetch.start()
    columns = own_ref.shape[1] // 2
    count = items.shape[0] // 4

    widest = jnp.zeros((), f32)
    for ref in (own_ref, *(source_refs if kind != "own" else ())):
        widest = jnp.maximum(widest, jnp.max(jnp.abs(ref[0:3] - 0.5)))
    calm = widest < near

    def read(n):
        return items[4 * n], items[4 * n + 1], items[4 * n + 2], items[4 * n + 3]

    @pl.when(calm)
    def _():
        acc[...] = jnp.zeros_like(acc)
        if kind == "own":
            left, sums = feats

            def some(i, _):
                stage_sources(own_ref, i, rows, 0)
                for j in range(8):
                    left[i * 8 + j] = staged(rows, 0, j, 0, 48).T.astype(bf16)
                    sums[i * 8 + j] = staged(rows, 0, j, 48, 16).astype(bf16)
                return 0

            lax.fori_loop(0, own_ref.shape[1] // 8, some, 0)
        elif kind == "caps":
            left_caps, sums_caps = feats

            def some(i, _):
                for side in range(2):
                    stage_sources(source_refs[side], i, rows, side * 512)
                for j in range(8):
                    both = [staged(rows, side * 512, j, 0, 48) for side in range(2)]
                    left_caps[i * 8 + j] = jnp.concatenate(both, axis=0).T.astype(bf16)
                    both = [staged(rows, side * 512, j, 48, 16) for side in range(2)]
                    sums_caps[i * 8 + j] = jnp.concatenate(both, axis=0).astype(bf16)
                return 0

            lax.fori_loop(0, source_refs[0].shape[1] // 8, some, 0)
        else:
            left, sums, left_caps, sums_caps = feats
            base = 0
            for ref in source_refs:

                def some(i, _, ref=ref, base=base):
                    stage_sources(ref, i, rows, 0)
                    for c in range(2):
                        column = base + i * 2 + c
                        for z in range(2):
                            left[column * 2 + z] = staged(rows, 0, 4 * c + 1 + z, 0, 48).T.astype(bf16)
                            sums[column * 2 + z] = staged(rows, 0, 4 * c + 1 + z, 48, 16).astype(bf16)
                        both = [staged(rows, 0, 4 * c + 3 * side, 0, 48) for side in range(2)]
                        left_caps[column] = jnp.concatenate(both, axis=0).T.astype(bf16)
                        both = [staged(rows, 0, 4 * c + 3 * side, 48, 16) for side in range(2)]
                        sums_caps[column] = jnp.concatenate(both, axis=0).astype(bf16)
                    return 0

                lax.fori_loop(0, ref.shape[1] // 8, some, 0)
                base += ref.shape[1] // 4
        if kind == "own":
            stage_targets(own_ref, rows, right)
        fetch.wait()

        def some_items(g, _):
            for k in range(group):
                column, source, ox, oy = read(g * group + k)
                me = jnp.minimum(column, columns - 1) * 2
                side = [[jnp.concatenate([right[me + t, ox], right[me + t, 3 + oy], right[me + t, 6 + oz]], axis=0)
                         for oz in range(3)] for t in range(2)]
                got = None
                zed = None
                if kind != "caps":
                    low = weighted(left[source * 2], jnp.concatenate([side[0][1], side[1][0]], axis=1), sums[source * 2])
                    high = weighted(left[source * 2 + 1], jnp.concatenate([side[0][2], side[1][1]], axis=1), sums[source * 2 + 1])
                    got = low + high
                    zed = jnp.concatenate([high[:8, :128], -low[:8, 128:]], axis=1)
                if kind != "own":
                    blank = jnp.zeros_like(side[0][0])
                    right_caps = jnp.concatenate(
                        [jnp.concatenate([side[0][0], blank], axis=1), jnp.concatenate([blank, side[1][2]], axis=1)], axis=0
                    )
                    caps = weighted(left_caps[source], right_caps, sums_caps[source])
                    caps_got = jnp.concatenate([caps[:16, :128], caps[16:, 128:]], axis=1)
                    caps_zed = jnp.concatenate([-caps[:8, :128], caps[16:24, 128:]], axis=1)
                    got = caps_got if got is None else got + caps_got
                    zed = caps_zed if zed is None else zed + caps_zed
                head = got[:8]
                for t in range(2):
                    lanes = slice(128 * t, 128 * t + 128)
                    first = pl.multiple_of((t * (columns + 1) + column) * 40, 8)
                    acc[pl.ds(first, 16), :] += got[:, lanes]
                    acc[pl.ds(first + 16, 8), :] += (ox - 1).astype(f32) * head[:, lanes]
                    acc[pl.ds(first + 24, 8), :] += (oy - 1).astype(f32) * head[:, lanes]
                    acc[pl.ds(first + 32, 8), :] += zed[:, lanes]
            return 0

        lax.fori_loop(0, count // group, some_items, 0)

        def finish(i, _):
            for t in range(2):
                def row(r):
                    return acc[pl.ds((t * (columns + 1) + i * 8) * 40 + r, 8, stride=40), :]

                spot = pl.ds(i * 16 + t, 8, stride=2)
                total = row(0) + row(1) + row(2)
                for d in range(3):
                    moment = row(3 * d + 3) + row(3 * d + 4) + row(3 * d + 5)
                    moment = moment + (row(16 + 8 * d) + row(17 + 8 * d) + row(18 + 8 * d))
                    value = moment - (own_ref[d, spot, :] - 0.5) * total
                    if before is not None:
                        value = value + before[d, spot, :]
                    out_ref[d, spot, :] = value
            return 0

        lax.fori_loop(0, columns // 8, finish, 0)

    @pl.when(jnp.logical_not(calm))
    def _():
        fetch.wait()
        raw[...] = jnp.zeros_like(raw)
        base = 0
        for ref in source_refs:

            def keep(cell, _, ref=ref, base=base):
                for d in range(4):
                    raw[base + cell, d:d + 1, :] = ref[d, pl.ds(cell, 1), :]
                return 0

            lax.fori_loop(0, ref.shape[1], keep, 0)
            base += ref.shape[1]
        out_ref[...] = before[...] if before is not None else jnp.zeros_like(out_ref)
        layers = {"own": (1, 2), "caps": (0, 3), "rim": (0, 1, 2, 3)}[kind]

        def one(n, _):
            column, source, ox, oy = read(n)

            @pl.when(column < columns)
            def _():
                for layer in layers:
                    cell = {"own": source * 2 + layer - 1, "caps": source + (layer // 3) * columns, "rim": source * 4 + layer}[kind]
                    lined = raw[cell].T
                    for t in range(2):
                        if abs(layer - 1 - t) > 1:
                            continue
                        spot = pl.ds(column * 2 + t, 1)
                        offset = ((ox - 1).astype(f32), (oy - 1).astype(f32), float(layer - 1 - t))
                        away = [(lined[:, d:d + 1] + offset[d]) - own_ref[d, spot, :] for d in range(3)]
                        q = away[0] * away[0] + away[1] * away[1] + away[2] * away[2]
                        r = lax.rsqrt(q + soft_sq)
                        taper = jnp.maximum(1.0 - q * (1.0 / cut_sq), 0.0)
                        w = lined[:, 3:4] * (r * r * r) * (taper * taper)
                        for d in range(3):
                            out_ref[d, spot, :] += jnp.sum(w * away[d], axis=0, keepdims=True)
            return 0

        lax.fori_loop(0, count, one, 0)


def listed(grid, kind):
    nx, ny = grid
    found = []
    for tx in range(nx):
        for ty in range(ny):
            for ox in range(3):
                for oy in range(3):
                    x, y = tx + ox - 1, ty + oy - 1
                    inside = 0 <= x < nx and 0 <= y < ny
                    if inside and kind != "rim":
                        found.append((tx * ny + ty, x * ny + y, ox, oy))
                    elif not inside and kind == "rim":
                        beyond = int(x >= nx)
                        if 0 <= x < nx:
                            source = x if y < 0 else nx + x
                        elif 0 <= y < ny:
                            source = 2 * nx + beyond * ny + y
                        else:
                            source = 2 * nx + 2 * ny + 2 * int(y >= ny) + beyond
                        found.append((tx * ny + ty, source, ox, oy))
    return found


def pull(kind, group, grid, own, source_arrays=(), right=None, before=None):
    nx, ny = grid
    columns = nx * ny
    items = listed(grid, kind)
    while len(items) % group:
        items.append((columns, 0, 1, 1))
    table = np.asarray(items, np.int32).reshape(-1)
    cells = sum(a.shape[1] for a in source_arrays) if source_arrays else own.shape[1]
    middle = {"own": cells, "caps": 0, "rim": cells // 2}[kind]
    capped = {"own": 0, "caps": cells // 2, "rim": cells // 4}[kind]
    feats = []
    if middle:
        feats += [pltpu.VMEM((middle, 128, 48), bf16), pltpu.VMEM((middle, 16, 128), bf16)]
    if capped:
        feats += [pltpu.VMEM((capped, 128, 96), bf16), pltpu.VMEM((capped, 32, 128), bf16)]
    args = [own, *source_arrays] + ([right, before] if source_arrays else [])
    out = jax.ShapeDtypeStruct((3, own.shape[1], 128), f32)
    made = jax.ShapeDtypeStruct((own.shape[1], 9, 16, 128), bf16)
    in_vmem = pl.BlockSpec(memory_space=pltpu.VMEM)
    pairs = len(items) * (3 if kind == "rim" else 2 if kind == "own" else 1) * 128 * 256
    return pl.pallas_call(
        functools.partial(pull_kernel, (kind, group)),
        out_shape=out if source_arrays else (out, made),
        in_specs=[pl.BlockSpec(memory_space=pltpu.HBM)] + [in_vmem] * len(args),
        out_specs=in_vmem if source_arrays else (in_vmem, in_vmem),
        scratch_shapes=[
            pltpu.VMEM((1024, 128), f32),
            pltpu.VMEM((2 * (columns + 1) * 40, 128), f32),
            pltpu.VMEM((cells, 8, 128), f32),
            pltpu.SMEM(table.shape, jnp.int32),
            pltpu.SemaphoreType.DMA,
            *feats,
        ],
        compiler_params=pltpu.CompilerParams(vmem_limit_bytes=40 * 2**20),
        cost_estimate=pl.CostEstimate(flops=pairs * 40, bytes_accessed=2**20, transcendentals=pairs),
        name="pull_" + kind,
    )(jnp.asarray(table), *args)


def rolled(axes, step, cells):
    counts = [lax.axis_size(axis) for axis in axes]
    spots = list(np.ndindex(*counts))
    perm = []
    for spot in spots:
        goal = tuple((i + d) % n for i, d, n in zip(spot, step, counts))
        perm.append((spots.index(spot), spots.index(goal)))
    return lax.ppermute(cells, axes, perm)


def rolled_x(cells, axes=("gx",), step=()):
    if lax.axis_size("gx") == 2:
        return rolled(axes, (1, *step), cells)
    return jnp.concatenate([rolled(axes, (1, *step), cells[:, :1]), rolled(axes, (-1, *step), cells[:, 1:])], axis=1)


def pull_field(own):
    grid = own.shape[1:3]
    slots = own.shape[-1]

    def lined(cells):
        return cells.reshape(4, -1, slots)

    lower = rolled(("gz",), (1,), own[:, :, :, -1:])
    upper = rolled(("gz",), (-1,), own[:, :, :, :1])
    total, right = pull("own", 22, grid, lined(own))
    lower, upper, total = lax.optimization_barrier((lower, upper, total))

    def tall(*where):
        where = (slice(None), *where)
        return jnp.concatenate([lower[where], own[where], upper[where]], axis=3)

    every, first, last = slice(None), slice(0, 1), slice(-1, None)
    front = rolled(("gy",), (1,), tall(every, last))
    back = rolled(("gy",), (-1,), tall(every, first))
    sides = rolled_x(jnp.concatenate([tall(last), tall(first)], axis=1))
    corners = [
        rolled_x(jnp.concatenate([tall(last, row), tall(first, row)], axis=1), ("gx", "gy"), (step,))
        for step, row in ((1, last), (-1, first))
    ]
    total = pull("caps", 55, grid, lined(own), [lined(lower), lined(upper)], right, total)
    rim = (front, back, sides, *corners)
    rim, total = lax.optimization_barrier((rim, total))
    total = pull("rim", 17, grid, lined(own), [lined(cells) for cells in rim], right, total)
    return total.reshape(3, *own.shape[1:])


def body(halo_position, halo_velocity, halo_mass, cell_counts):
    occupied = lax.broadcasted_iota(jnp.int32, halo_mass.shape, 3) < cell_counts[..., None]
    held_mass = jnp.where(occupied, halo_mass, 0.0)[None]
    own = lax.optimization_barrier(jnp.concatenate([halo_position, held_mass], axis=0))
    first_pull = pull_field(own)
    drifted = jnp.where(occupied[None], halo_position + halo_velocity + 0.5 * first_pull, 0.0)
    own = lax.optimization_barrier(jnp.concatenate([drifted, own[3:]], axis=0))
    second_pull = pull_field(own)
    predicted = halo_position + halo_velocity + first_pull / 3.0 + second_pull / 6.0
    return jnp.where(occupied[None], predicted, 0.0)


def solution(mesh):
    return jax.shard_map(
        body,
        mesh=mesh,
        in_specs=(
            P(None, "gx", "gy", "gz", None),
            P(None, "gx", "gy", "gz", None),
            P("gx", "gy", "gz", None),
            P("gx", "gy", "gz"),
        ),
        out_specs=P(None, "gx", "gy", "gz", None),
        check_vma=False,
    )
```

```python
import functools
import jax
import jax.numpy as jnp
import numpy as np
from jax import lax
from jax.experimental import pallas as pl
from jax.experimental.pallas import tpu as pltpu
from jax.sharding import PartitionSpec as P

soft_sq = 0.01
cut_sq = 0.64
near = 6.0
f32, bf16 = jnp.float32, jnp.bfloat16


def rounded(v):
    return v.astype(bf16).astype(f32)


def split3(v):
    a = rounded(v)
    rest = v - a
    b = rounded(rest)
    return a, b, rest - b


def squares(v, extra=0.0):
    a = rounded(v)
    rest = v - a
    b = rounded(rest)
    top = a * a
    top_a = rounded(top)
    low = 2.0 * a * rest + rest * rest + extra
    return (a, b, rest - b), (top_a, top - top_a, *split3(low))


def source_rows(v):
    (a, b, c), (pa, pb, pc, pd, pe) = squares(v)
    one = jnp.ones_like(v)
    return [a, one, one, pa, pb, a, b, b, a, c, one, one, one, pc, pd, pe]


def target_rows(v, extra):
    (a, b, c), (pa, pb, pc, pd, pe) = squares(v, extra)
    one = jnp.ones_like(v)
    return [-2.0 * a, pa, pb, one, one, -2.0 * b, -2.0 * a, -2.0 * b, -2.0 * c, -2.0 * a, pc, pd, pe, one, one, one]


def stage_sources(ref, i, rows, base):
    at = pl.ds(pl.multiple_of(i * 8, 8), 8)
    pieces = []
    mass = ref[3, at, :] * (1.0 / (cut_sq * cut_sq))
    sums = list(split3(mass))
    for d in range(3):
        place = ref[d, at, :] - 0.5
        pieces += source_rows(place)
        sums += list(split3(mass * place))
    for k, piece in enumerate(pieces + sums):
        rows[base + k * 8:base + k * 8 + 8, :] = piece


def staged(rows, base, j, first, count):
    return rows[pl.ds(base + first * 8 + j, count, stride=8), :]


def stage_targets(own_ref, rows, right):
    def some(i, _):
        at = pl.ds(pl.multiple_of(i * 8, 8), 8)
        for d in range(3):
            base = own_ref[d, at, :] - 0.5
            for o in range(3):
                for k, piece in enumerate(target_rows(base - float(o - 1), soft_sq if d == 2 else 0.0)):
                    rows[k * 8:k * 8 + 8, :] = piece
                for j in range(8):
                    right[i * 8 + j, d * 3 + o] = staged(rows, 0, j, 0, 16).astype(bf16)
        return 0

    lax.fori_loop(0, own_ref.shape[1] // 8, some, 0)


def weighted(left, right, moments):
    q = jnp.dot(left, right, preferred_element_type=f32)
    r = lax.rsqrt(q)
    t = jnp.maximum((cut_sq + soft_sq) - q, 0.0) * r
    w = t * t * r
    hi = w.astype(bf16)
    lo = (w - hi.astype(f32)).astype(bf16)
    return jnp.dot(
        jnp.concatenate([moments, moments], axis=1), jnp.concatenate([hi, lo], axis=0), preferred_element_type=f32
    )


def pull_kernel(plan, *refs):
    kind, group = plan
    own_ref = refs[1]
    sources = {"own": 0, "caps": 2, "rim": 5}[kind]
    at = 2 + sources
    source_refs = refs[2:at] or refs[1:2]
    before = None
    if kind == "own":
        out_ref, right = refs[at:at + 2]
    else:
        right, before, out_ref = refs[at:at + 3]
        at += 1
    rows, acc, raw, items, copied, *feats = refs[at + 2:]
    fetch = pltpu.make_async_copy(refs[0], items, copied)
    fetch.start()
    columns = own_ref.shape[1] // 2
    count = items.shape[0] // 4

    widest = jnp.zeros((), f32)
    for ref in (own_ref, *(source_refs if kind != "own" else ())):
        widest = jnp.maximum(widest, jnp.max(jnp.abs(ref[0:3] - 0.5)))
    calm = widest < near

    def read(n):
        return items[4 * n], items[4 * n + 1], items[4 * n + 2], items[4 * n + 3]

    @pl.when(calm)
    def _():
        acc[...] = jnp.zeros_like(acc)
        if kind == "own":
            left, sums = feats

            def some(i, _):
                stage_sources(own_ref, i, rows, 0)
                for j in range(8):
                    left[i * 8 + j] = staged(rows, 0, j, 0, 48).T.astype(bf16)
                    sums[i * 8 + j] = staged(rows, 0, j, 48, 16).astype(bf16)
                return 0

            lax.fori_loop(0, own_ref.shape[1] // 8, some, 0)
        elif kind == "caps":
            left_caps, sums_caps = feats

            def some(i, _):
                for side in range(2):
                    stage_sources(source_refs[side], i, rows, side * 512)
                for j in range(8):
                    both = [staged(rows, side * 512, j, 0, 48) for side in range(2)]
                    left_caps[i * 8 + j] = jnp.concatenate(both, axis=0).T.astype(bf16)
                    both = [staged(rows, side * 512, j, 48, 16) for side in range(2)]
                    sums_caps[i * 8 + j] = jnp.concatenate(both, axis=0).astype(bf16)
                return 0

            lax.fori_loop(0, source_refs[0].shape[1] // 8, some, 0)
        else:
            left, sums, left_caps, sums_caps = feats
            base = 0
            for ref in source_refs:

                def some(i, _, ref=ref, base=base):
                    stage_sources(ref, i, rows, 0)
                    for c in range(2):
                        column = base + i * 2 + c
                        for z in range(2):
                            left[column * 2 + z] = staged(rows, 0, 4 * c + 1 + z, 0, 48).T.astype(bf16)
                            sums[column * 2 + z] = staged(rows, 0, 4 * c + 1 + z, 48, 16).astype(bf16)
                        both = [staged(rows, 0, 4 * c + 3 * side, 0, 48) for side in range(2)]
                        left_caps[column] = jnp.concatenate(both, axis=0).T.astype(bf16)
                        both = [staged(rows, 0, 4 * c + 3 * side, 48, 16) for side in range(2)]
                        sums_caps[column] = jnp.concatenate(both, axis=0).astype(bf16)
                    return 0

                lax.fori_loop(0, ref.shape[1] // 8, some, 0)
                base += ref.shape[1] // 4
        if kind == "own":
            stage_targets(own_ref, rows, right)
        fetch.wait()

        def some_items(g, _):
            for k in range(group):
                column, source, ox, oy = read(g * group + k)
                me = jnp.minimum(column, columns - 1) * 2
                side = [[jnp.concatenate([right[me + t, ox], right[me + t, 3 + oy], right[me + t, 6 + oz]], axis=0)
                         for oz in range(3)] for t in range(2)]
                got = None
                zed = None
                if kind != "caps":
                    low = weighted(left[source * 2], jnp.concatenate([side[0][1], side[1][0]], axis=1), sums[source * 2])
                    high = weighted(left[source * 2 + 1], jnp.concatenate([side[0][2], side[1][1]], axis=1), sums[source * 2 + 1])
                    got = low + high
                    zed = jnp.concatenate([high[:8, :128], -low[:8, 128:]], axis=1)
                if kind != "own":
                    blank = jnp.zeros_like(side[0][0])
                    right_caps = jnp.concatenate(
                        [jnp.concatenate([side[0][0], blank], axis=1), jnp.concatenate([blank, side[1][2]], axis=1)], axis=0
                    )
                    caps = weighted(left_caps[source], right_caps, sums_caps[source])
                    caps_got = jnp.concatenate([caps[:16, :128], caps[16:, 128:]], axis=1)
                    caps_zed = jnp.concatenate([-caps[:8, :128], caps[16:24, 128:]], axis=1)
                    got = caps_got if got is None else got + caps_got
                    zed = caps_zed if zed is None else zed + caps_zed
                head = got[:8]
                for t in range(2):
                    lanes = slice(128 * t, 128 * t + 128)
                    first = pl.multiple_of((t * (columns + 1) + column) * 40, 8)
                    acc[pl.ds(first, 16), :] += got[:, lanes]
                    acc[pl.ds(first + 16, 8), :] += (ox - 1).astype(f32) * head[:, lanes]
                    acc[pl.ds(first + 24, 8), :] += (oy - 1).astype(f32) * head[:, lanes]
                    acc[pl.ds(first + 32, 8), :] += zed[:, lanes]
            return 0

        lax.fori_loop(0, count // group, some_items, 0)

        def finish(i, _):
            for t in range(2):
                def row(r):
                    return acc[pl.ds((t * (columns + 1) + i * 8) * 40 + r, 8, stride=40), :]

                spot = pl.ds(i * 16 + t, 8, stride=2)
                total = row(0) + row(1) + row(2)
                for d in range(3):
                    moment = row(3 * d + 3) + row(3 * d + 4) + row(3 * d + 5)
                    moment = moment + (row(16 + 8 * d) + row(17 + 8 * d) + row(18 + 8 * d))
                    value = moment - (own_ref[d, spot, :] - 0.5) * total
                    if before is not None:
                        value = value + before[d, spot, :]
                    out_ref[d, spot, :] = value
            return 0

        lax.fori_loop(0, columns // 8, finish, 0)

    @pl.when(jnp.logical_not(calm))
    def _():
        fetch.wait()
        raw[...] = jnp.zeros_like(raw)
        base = 0
        for ref in source_refs:

            def keep(cell, _, ref=ref, base=base):
                for d in range(4):
                    raw[base + cell, d:d + 1, :] = ref[d, pl.ds(cell, 1), :]
                return 0

            lax.fori_loop(0, ref.shape[1], keep, 0)
            base += ref.shape[1]
        out_ref[...] = before[...] if before is not None else jnp.zeros_like(out_ref)
        layers = {"own": (1, 2), "caps": (0, 3), "rim": (0, 1, 2, 3)}[kind]

        def one(n, _):
            column, source, ox, oy = read(n)

            @pl.when(column < columns)
            def _():
                for layer in layers:
                    cell = {"own": source * 2 + layer - 1, "caps": source + (layer // 3) * columns, "rim": source * 4 + layer}[kind]
                    lined = raw[cell].T
                    for t in range(2):
                        if abs(layer - 1 - t) > 1:
                            continue
                        spot = pl.ds(column * 2 + t, 1)
                        offset = ((ox - 1).astype(f32), (oy - 1).astype(f32), float(layer - 1 - t))
                        away = [(lined[:, d:d + 1] + offset[d]) - own_ref[d, spot, :] for d in range(3)]
                        q = away[0] * away[0] + away[1] * away[1] + away[2] * away[2]
                        r = lax.rsqrt(q + soft_sq)
                        taper = jnp.maximum(1.0 - q * (1.0 / cut_sq), 0.0)
                        w = lined[:, 3:4] * (r * r * r) * (taper * taper)
                        for d in range(3):
                            out_ref[d, spot, :] += jnp.sum(w * away[d], axis=0, keepdims=True)
            return 0

        lax.fori_loop(0, count, one, 0)


def listed(grid, kind):
    nx, ny = grid
    found = []
    for tx in range(nx):
        for ty in range(ny):
            for ox in range(3):
                for oy in range(3):
                    x, y = tx + ox - 1, ty + oy - 1
                    inside = 0 <= x < nx and 0 <= y < ny
                    if inside and kind != "rim":
                        found.append((tx * ny + ty, x * ny + y, ox, oy))
                    elif not inside and kind == "rim":
                        beyond = int(x >= nx)
                        if 0 <= x < nx:
                            source = x if y < 0 else nx + x
                        elif 0 <= y < ny:
                            source = 2 * nx + beyond * ny + y
                        else:
                            source = 2 * nx + 2 * ny + 2 * int(y >= ny) + beyond
                        found.append((tx * ny + ty, source, ox, oy))
    return found


def pull(kind, group, grid, own, source_arrays=(), right=None, before=None):
    nx, ny = grid
    columns = nx * ny
    items = listed(grid, kind)
    while len(items) % group:
        items.append((columns, 0, 1, 1))
    table = np.asarray(items, np.int32).reshape(-1)
    cells = sum(a.shape[1] for a in source_arrays) if source_arrays else own.shape[1]
    middle = {"own": cells, "caps": 0, "rim": cells // 2}[kind]
    capped = {"own": 0, "caps": cells // 2, "rim": cells // 4}[kind]
    feats = []
    if middle:
        feats += [pltpu.VMEM((middle, 128, 48), bf16), pltpu.VMEM((middle, 16, 128), bf16)]
    if capped:
        feats += [pltpu.VMEM((capped, 128, 96), bf16), pltpu.VMEM((capped, 32, 128), bf16)]
    args = [own, *source_arrays] + ([right, before] if source_arrays else [])
    out = jax.ShapeDtypeStruct((3, own.shape[1], 128), f32)
    made = jax.ShapeDtypeStruct((own.shape[1], 9, 16, 128), bf16)
    in_vmem = pl.BlockSpec(memory_space=pltpu.VMEM)
    pairs = len(items) * (3 if kind == "rim" else 2 if kind == "own" else 1) * 128 * 256
    return pl.pallas_call(
        functools.partial(pull_kernel, (kind, group)),
        out_shape=out if source_arrays else (out, made),
        in_specs=[pl.BlockSpec(memory_space=pltpu.HBM)] + [in_vmem] * len(args),
        out_specs=in_vmem if source_arrays else (in_vmem, in_vmem),
        scratch_shapes=[
            pltpu.VMEM((1024, 128), f32),
            pltpu.VMEM((2 * (columns + 1) * 40, 128), f32),
            pltpu.VMEM((cells, 8, 128), f32),
            pltpu.SMEM(table.shape, jnp.int32),
            pltpu.SemaphoreType.DMA,
            *feats,
        ],
        compiler_params=pltpu.CompilerParams(vmem_limit_bytes=40 * 2**20),
        cost_estimate=pl.CostEstimate(flops=pairs * 40, bytes_accessed=2**20, transcendentals=pairs),
        name="pull_" + kind,
    )(jnp.asarray(table), *args)


def rolled(axes, step, cells):
    counts = [lax.axis_size(axis) for axis in axes]
    spots = list(np.ndindex(*counts))
    perm = []
    for spot in spots:
        goal = tuple((i + d) % n for i, d, n in zip(spot, step, counts))
        perm.append((spots.index(spot), spots.index(goal)))
    return lax.ppermute(cells, axes, perm)


def rolled_x(cells, axes=("gx",), step=()):
    if lax.axis_size("gx") == 2:
        return rolled(axes, (1, *step), cells)
    return jnp.concatenate([rolled(axes, (1, *step), cells[:, :1]), rolled(axes, (-1, *step), cells[:, 1:])], axis=1)


def pull_field(own):
    grid = own.shape[1:3]
    slots = own.shape[-1]

    def lined(cells):
        return cells.reshape(4, -1, slots)

    lower = rolled(("gz",), (1,), own[:, :, :, -1:])
    upper = rolled(("gz",), (-1,), own[:, :, :, :1])
    total, right = pull("own", 44, grid, lined(own))
    lower, upper, total = lax.optimization_barrier((lower, upper, total))

    def tall(*where):
        where = (slice(None), *where)
        return jnp.concatenate([lower[where], own[where], upper[where]], axis=3)

    every, first, last = slice(None), slice(0, 1), slice(-1, None)
    front = rolled(("gy",), (1,), tall(every, last))
    back = rolled(("gy",), (-1,), tall(every, first))
    sides = rolled_x(jnp.concatenate([tall(last), tall(first)], axis=1))
    corners = [
        rolled_x(jnp.concatenate([tall(last, row), tall(first, row)], axis=1), ("gx", "gy"), (step,))
        for step, row in ((1, last), (-1, first))
    ]
    total = pull("caps", 110, grid, lined(own), [lined(lower), lined(upper)], right, total)
    rim = (front, back, sides, *corners)
    rim, total = lax.optimization_barrier((rim, total))
    total = pull("rim", 34, grid, lined(own), [lined(cells) for cells in rim], right, total)
    return total.reshape(3, *own.shape[1:])


def body(halo_position, halo_velocity, halo_mass, cell_counts):
    occupied = lax.broadcasted_iota(jnp.int32, halo_mass.shape, 3) < cell_counts[..., None]
    held_mass = jnp.where(occupied, halo_mass, 0.0)[None]
    own = lax.optimization_barrier(jnp.concatenate([halo_position, held_mass], axis=0))
    first_pull = pull_field(own)
    drifted = jnp.where(occupied[None], halo_position + halo_velocity + 0.5 * first_pull, 0.0)
    own = lax.optimization_barrier(jnp.concatenate([drifted, own[3:]], axis=0))
    second_pull = pull_field(own)
    predicted = halo_position + halo_velocity + first_pull / 3.0 + second_pull / 6.0
    return jnp.where(occupied[None], predicted, 0.0)


def solution(mesh):
    return jax.shard_map(
        body,
        mesh=mesh,
        in_specs=(
            P(None, "gx", "gy", "gz", None),
            P(None, "gx", "gy", "gz", None),
            P("gx", "gy", "gz", None),
            P("gx", "gy", "gz"),
        ),
        out_specs=P(None, "gx", "gy", "gz", None),
        check_vma=False,
    )
```

```python
import functools
import jax
import jax.numpy as jnp
import numpy as np
from jax import lax
from jax.experimental import pallas as pl
from jax.experimental.pallas import tpu as pltpu
from jax.sharding import PartitionSpec as P

soft_sq = 0.01
cut_sq = 0.64
near = 6.0
f32, bf16 = jnp.float32, jnp.bfloat16


def rounded(v):
    return v.astype(bf16).astype(f32)


def split3(v):
    a = rounded(v)
    rest = v - a
    b = rounded(rest)
    return a, b, rest - b


def squares(v, extra=0.0):
    a = rounded(v)
    rest = v - a
    b = rounded(rest)
    top = a * a
    top_a = rounded(top)
    low = 2.0 * a * rest + rest * rest + extra
    return (a, b, rest - b), (top_a, top - top_a, *split3(low))


def source_rows(v):
    (a, b, c), (pa, pb, pc, pd, pe) = squares(v)
    one = jnp.ones_like(v)
    return [a, one, one, pa, pb, a, b, b, a, c, one, one, one, pc, pd, pe]


def target_rows(v, extra):
    (a, b, c), (pa, pb, pc, pd, pe) = squares(v, extra)
    one = jnp.ones_like(v)
    return [-2.0 * a, pa, pb, one, one, -2.0 * b, -2.0 * a, -2.0 * b, -2.0 * c, -2.0 * a, pc, pd, pe, one, one, one]


def stage_sources(ref, i, rows, base):
    at = pl.ds(pl.multiple_of(i * 8, 8), 8)
    pieces = []
    mass = ref[3, at, :] * (1.0 / (cut_sq * cut_sq))
    sums = list(split3(mass))
    for d in range(3):
        place = ref[d, at, :] - 0.5
        pieces += source_rows(place)
        sums += list(split3(mass * place))
    for k, piece in enumerate(pieces + sums):
        rows[base + k * 8:base + k * 8 + 8, :] = piece


def staged(rows, base, j, first, count):
    return rows[pl.ds(base + first * 8 + j, count, stride=8), :]


def stage_targets(own_ref, rows, right):
    def some(i, _):
        at = pl.ds(pl.multiple_of(i * 8, 8), 8)
        for d in range(3):
            base = own_ref[d, at, :] - 0.5
            for o in range(3):
                where = (d * 3 + o) * 128
                for k, piece in enumerate(target_rows(base - float(o - 1), soft_sq if d == 2 else 0.0)):
                    rows[where + k * 8:where + k * 8 + 8, :] = piece
                for j in range(8):
                    right[i * 8 + j, d * 3 + o] = staged(rows, where, j, 0, 16).astype(bf16)
        return 0

    lax.fori_loop(0, own_ref.shape[1] // 8, some, 0)


def weighted(left, right, moments):
    q = jnp.dot(left, right, preferred_element_type=f32)
    r = lax.rsqrt(q)
    t = jnp.maximum((cut_sq + soft_sq) - q, 0.0) * r
    w = t * t * r
    hi = w.astype(bf16)
    lo = (w - hi.astype(f32)).astype(bf16)
    return jnp.dot(
        jnp.concatenate([moments, moments], axis=1), jnp.concatenate([hi, lo], axis=0), preferred_element_type=f32
    )


def paired(count, step):
    def two(i, _):
        step(2 * i, 0)
        step(2 * i + 1, 1)
        return 0

    lax.fori_loop(0, count // 2, two, 0)
    if count % 2:
        step(count - 1, 0)


def pull_kernel(plan, *refs):
    kind, group = plan
    own_ref = refs[1]
    sources = {"own": 0, "caps": 2, "rim": 5}[kind]
    at = 2 + sources
    source_refs = refs[2:at] or refs[1:2]
    before = None
    if kind == "own":
        out_ref, right = refs[at:at + 2]
    else:
        right, before, out_ref = refs[at:at + 3]
        at += 1
    rows, acc, raw, items, copied, *feats = refs[at + 2:]
    fetch = pltpu.make_async_copy(refs[0], items, copied)
    fetch.start()
    columns = own_ref.shape[1] // 2
    count = items.shape[0] // 4

    widest = jnp.zeros((), f32)
    for ref in (own_ref, *(source_refs if kind != "own" else ())):
        widest = jnp.maximum(widest, jnp.max(jnp.abs(ref[0:3] - 0.5)))
    calm = widest < near

    def read(n):
        return items[4 * n], items[4 * n + 1], items[4 * n + 2], items[4 * n + 3]

    @pl.when(calm)
    def _():
        acc[...] = jnp.zeros_like(acc)
        if kind == "own":
            left, sums = feats

            def some(i, lane):
                base = lane * 512
                stage_sources(own_ref, i, rows, base)
                for j in range(8):
                    left[i * 8 + j] = staged(rows, base, j, 0, 48).T.astype(bf16)
                    sums[i * 8 + j] = staged(rows, base, j, 48, 16).astype(bf16)

            paired(own_ref.shape[1] // 8, some)
        elif kind == "caps":
            left_caps, sums_caps = feats

            def some(i, lane):
                bases = [lane * 1024, lane * 1024 + 512]
                for ref, base in zip(source_refs, bases):
                    stage_sources(ref, i, rows, base)
                for j in range(8):
                    both = [staged(rows, base, j, 0, 48) for base in bases]
                    left_caps[i * 8 + j] = jnp.concatenate(both, axis=0).T.astype(bf16)
                    both = [staged(rows, base, j, 48, 16) for base in bases]
                    sums_caps[i * 8 + j] = jnp.concatenate(both, axis=0).astype(bf16)

            paired(source_refs[0].shape[1] // 8, some)
        else:
            left, sums, left_caps, sums_caps = feats
            base = 0
            for ref in source_refs:

                def some(i, lane, ref=ref, base=base):
                    where = lane * 512
                    stage_sources(ref, i, rows, where)
                    for c in range(2):
                        column = base + i * 2 + c
                        for z in range(2):
                            left[column * 2 + z] = staged(rows, where, 4 * c + 1 + z, 0, 48).T.astype(bf16)
                            sums[column * 2 + z] = staged(rows, where, 4 * c + 1 + z, 48, 16).astype(bf16)
                        both = [staged(rows, where, 4 * c + 3 * side, 0, 48) for side in range(2)]
                        left_caps[column] = jnp.concatenate(both, axis=0).T.astype(bf16)
                        both = [staged(rows, where, 4 * c + 3 * side, 48, 16) for side in range(2)]
                        sums_caps[column] = jnp.concatenate(both, axis=0).astype(bf16)

                paired(ref.shape[1] // 8, some)
                base += ref.shape[1] // 4
        if kind == "own":
            stage_targets(own_ref, rows, right)
        fetch.wait()

        def some_items(g, _):
            for k in range(group):
                column, source, ox, oy = read(g * group + k)
                me = jnp.minimum(column, columns - 1) * 2
                side = [[jnp.concatenate([right[me + t, ox], right[me + t, 3 + oy], right[me + t, 6 + oz]], axis=0)
                         for oz in range(3)] for t in range(2)]
                got = None
                zed = None
                if kind != "caps":
                    low = weighted(left[source * 2], jnp.concatenate([side[0][1], side[1][0]], axis=1), sums[source * 2])
                    high = weighted(left[source * 2 + 1], jnp.concatenate([side[0][2], side[1][1]], axis=1), sums[source * 2 + 1])
                    got = low + high
                    zed = jnp.concatenate([high[:8, :128], -low[:8, 128:]], axis=1)
                if kind != "own":
                    blank = jnp.zeros_like(side[0][0])
                    right_caps = jnp.concatenate(
                        [jnp.concatenate([side[0][0], blank], axis=1), jnp.concatenate([blank, side[1][2]], axis=1)], axis=0
                    )
                    caps = weighted(left_caps[source], right_caps, sums_caps[source])
                    caps_got = jnp.concatenate([caps[:16, :128], caps[16:, 128:]], axis=1)
                    caps_zed = jnp.concatenate([-caps[:8, :128], caps[16:24, 128:]], axis=1)
                    got = caps_got if got is None else got + caps_got
                    zed = caps_zed if zed is None else zed + caps_zed
                head = got[:8]
                for t in range(2):
                    lanes = slice(128 * t, 128 * t + 128)
                    first = pl.multiple_of((t * (columns + 1) + column) * 40, 8)
                    acc[pl.ds(first, 16), :] += got[:, lanes]
                    acc[pl.ds(first + 16, 8), :] += (ox - 1).astype(f32) * head[:, lanes]
                    acc[pl.ds(first + 24, 8), :] += (oy - 1).astype(f32) * head[:, lanes]
                    acc[pl.ds(first + 32, 8), :] += zed[:, lanes]
            return 0

        lax.fori_loop(0, count // group, some_items, 0)

        def finish(i, _):
            for t in range(2):
                def row(r):
                    return acc[pl.ds((t * (columns + 1) + i * 8) * 40 + r, 8, stride=40), :]

                spot = pl.ds(i * 16 + t, 8, stride=2)
                total = row(0) + row(1) + row(2)
                for d in range(3):
                    moment = row(3 * d + 3) + row(3 * d + 4) + row(3 * d + 5)
                    moment = moment + (row(16 + 8 * d) + row(17 + 8 * d) + row(18 + 8 * d))
                    value = moment - (own_ref[d, spot, :] - 0.5) * total
                    if before is not None:
                        value = value + before[d, spot, :]
                    out_ref[d, spot, :] = value
            return 0

        lax.fori_loop(0, columns // 8, finish, 0)

    @pl.when(jnp.logical_not(calm))
    def _():
        fetch.wait()
        raw[...] = jnp.zeros_like(raw)
        base = 0
        for ref in source_refs:

            def keep(cell, _, ref=ref, base=base):
                for d in range(4):
                    raw[base + cell, d:d + 1, :] = ref[d, pl.ds(cell, 1), :]
                return 0

            lax.fori_loop(0, ref.shape[1], keep, 0)
            base += ref.shape[1]
        out_ref[...] = before[...] if before is not None else jnp.zeros_like(out_ref)
        layers = {"own": (1, 2), "caps": (0, 3), "rim": (0, 1, 2, 3)}[kind]

        def one(n, _):
            column, source, ox, oy = read(n)

            @pl.when(column < columns)
            def _():
                for layer in layers:
                    cell = {"own": source * 2 + layer - 1, "caps": source + (layer // 3) * columns, "rim": source * 4 + layer}[kind]
                    lined = raw[cell].T
                    for t in range(2):
                        if abs(layer - 1 - t) > 1:
                            continue
                        spot = pl.ds(column * 2 + t, 1)
                        offset = ((ox - 1).astype(f32), (oy - 1).astype(f32), float(layer - 1 - t))
                        away = [(lined[:, d:d + 1] + offset[d]) - own_ref[d, spot, :] for d in range(3)]
                        q = away[0] * away[0] + away[1] * away[1] + away[2] * away[2]
                        r = lax.rsqrt(q + soft_sq)
                        taper = jnp.maximum(1.0 - q * (1.0 / cut_sq), 0.0)
                        w = lined[:, 3:4] * (r * r * r) * (taper * taper)
                        for d in range(3):
                            out_ref[d, spot, :] += jnp.sum(w * away[d], axis=0, keepdims=True)
            return 0

        lax.fori_loop(0, count, one, 0)


def listed(grid, kind):
    nx, ny = grid
    found = []
    for tx in range(nx):
        for ty in range(ny):
            for ox in range(3):
                for oy in range(3):
                    x, y = tx + ox - 1, ty + oy - 1
                    inside = 0 <= x < nx and 0 <= y < ny
                    if inside and kind != "rim":
                        found.append((tx * ny + ty, x * ny + y, ox, oy))
                    elif not inside and kind == "rim":
                        beyond = int(x >= nx)
                        if 0 <= x < nx:
                            source = x if y < 0 else nx + x
                        elif 0 <= y < ny:
                            source = 2 * nx + beyond * ny + y
                        else:
                            source = 2 * nx + 2 * ny + 2 * int(y >= ny) + beyond
                        found.append((tx * ny + ty, source, ox, oy))
    return found


def table_of(kind, group, grid):
    items = listed(grid, kind)
    while len(items) % group:
        items.append((grid[0] * grid[1], 0, 1, 1))
    return np.asarray(items, np.int32).reshape(-1)


def pull(kind, group, table, grid, own, source_arrays=(), right=None, before=None):
    nx, ny = grid
    columns = nx * ny
    cells = sum(a.shape[1] for a in source_arrays) if source_arrays else own.shape[1]
    middle = {"own": cells, "caps": 0, "rim": cells // 2}[kind]
    capped = {"own": 0, "caps": cells // 2, "rim": cells // 4}[kind]
    feats = []
    if middle:
        feats += [pltpu.VMEM((middle, 128, 48), bf16), pltpu.VMEM((middle, 16, 128), bf16)]
    if capped:
        feats += [pltpu.VMEM((capped, 128, 96), bf16), pltpu.VMEM((capped, 32, 128), bf16)]
    args = [own, *source_arrays] + ([right, before] if source_arrays else [])
    out = jax.ShapeDtypeStruct((3, own.shape[1], 128), f32)
    made = jax.ShapeDtypeStruct((own.shape[1], 9, 16, 128), bf16)
    in_vmem = pl.BlockSpec(memory_space=pltpu.VMEM)
    pairs = table.size // 4 * (3 if kind == "rim" else 2 if kind == "own" else 1) * 128 * 256
    return pl.pallas_call(
        functools.partial(pull_kernel, (kind, group)),
        out_shape=out if source_arrays else (out, made),
        in_specs=[pl.BlockSpec(memory_space=pltpu.HBM)] + [in_vmem] * len(args),
        out_specs=in_vmem if source_arrays else (in_vmem, in_vmem),
        scratch_shapes=[
            pltpu.VMEM((2048, 128), f32),
            pltpu.VMEM((2 * (columns + 1) * 40, 128), f32),
            pltpu.VMEM((cells, 8, 128), f32),
            pltpu.SMEM(table.shape, jnp.int32),
            pltpu.SemaphoreType.DMA,
            *feats,
        ],
        compiler_params=pltpu.CompilerParams(vmem_limit_bytes=40 * 2**20),
        cost_estimate=pl.CostEstimate(flops=pairs * 40, bytes_accessed=2**20, transcendentals=pairs),
        name="pull_" + kind,
    )(table, *args)


def rolled(axes, step, cells):
    counts = [lax.axis_size(axis) for axis in axes]
    spots = list(np.ndindex(*counts))
    perm = []
    for spot in spots:
        goal = tuple((i + d) % n for i, d, n in zip(spot, step, counts))
        perm.append((spots.index(spot), spots.index(goal)))
    return lax.ppermute(cells, axes, perm)


def rolled_x(cells, axes=("gx",), step=()):
    if lax.axis_size("gx") == 2:
        return rolled(axes, (1, *step), cells)
    return jnp.concatenate([rolled(axes, (1, *step), cells[:, :1]), rolled(axes, (-1, *step), cells[:, 1:])], axis=1)


groups = {"own": 44, "caps": 110, "rim": 34}


def pull_field(own, tables):
    grid = own.shape[1:3]
    slots = own.shape[-1]

    def lined(cells):
        return cells.reshape(4, -1, slots)

    lower = rolled(("gz",), (1,), own[:, :, :, -1:])
    upper = rolled(("gz",), (-1,), own[:, :, :, :1])
    total, right = pull("own", groups["own"], tables["own"], grid, lined(own))
    lower, upper, total = lax.optimization_barrier((lower, upper, total))

    def tall(*where):
        where = (slice(None), *where)
        return jnp.concatenate([lower[where], own[where], upper[where]], axis=3)

    every, first, last = slice(None), slice(0, 1), slice(-1, None)
    front = rolled(("gy",), (1,), tall(every, last))
    back = rolled(("gy",), (-1,), tall(every, first))
    sides = rolled_x(jnp.concatenate([tall(last), tall(first)], axis=1))
    corners = [
        rolled_x(jnp.concatenate([tall(last, row), tall(first, row)], axis=1), ("gx", "gy"), (step,))
        for step, row in ((1, last), (-1, first))
    ]
    total = pull("caps", groups["caps"], tables["caps"], grid, lined(own), [lined(lower), lined(upper)], right, total)
    rim = (front, back, sides, *corners)
    rim, total = lax.optimization_barrier((rim, total))
    total = pull("rim", groups["rim"], tables["rim"], grid, lined(own), [lined(cells) for cells in rim], right, total)
    return total.reshape(3, *own.shape[1:])


def body(halo_position, halo_velocity, halo_mass, cell_counts):
    occupied = lax.broadcasted_iota(jnp.int32, halo_mass.shape, 3) < cell_counts[..., None]
    held_mass = jnp.where(occupied, halo_mass, 0.0)[None]
    tables = {kind: jnp.asarray(table_of(kind, group, halo_mass.shape[:2])) for kind, group in groups.items()}
    own, tables = lax.optimization_barrier((jnp.concatenate([halo_position, held_mass], axis=0), tables))
    first_pull = pull_field(own, tables)
    drifted = jnp.where(occupied[None], halo_position + halo_velocity + 0.5 * first_pull, 0.0)
    own = lax.optimization_barrier(jnp.concatenate([drifted, own[3:]], axis=0))
    second_pull = pull_field(own, tables)
    predicted = halo_position + halo_velocity + first_pull / 3.0 + second_pull / 6.0
    return jnp.where(occupied[None], predicted, 0.0)


def solution(mesh):
    return jax.shard_map(
        body,
        mesh=mesh,
        in_specs=(
            P(None, "gx", "gy", "gz", None),
            P(None, "gx", "gy", "gz", None),
            P("gx", "gy", "gz", None),
            P("gx", "gy", "gz"),
        ),
        out_specs=P(None, "gx", "gy", "gz", None),
        check_vma=False,
    )
```

```python
import functools
import jax
import jax.numpy as jnp
import numpy as np
from jax import lax
from jax.experimental import pallas as pl
from jax.experimental.pallas import tpu as pltpu
from jax.sharding import PartitionSpec as P

soft_sq = 0.01
cut_sq = 0.64
near = 6.0
f32, bf16 = jnp.float32, jnp.bfloat16


def rounded(v):
    return v.astype(bf16).astype(f32)


def split3(v):
    a = rounded(v)
    rest = v - a
    b = rounded(rest)
    return a, b, rest - b


def squares(v, extra=0.0):
    a = rounded(v)
    rest = v - a
    b = rounded(rest)
    top = a * a
    top_a = rounded(top)
    low = 2.0 * a * rest + rest * rest + extra
    return (a, b, rest - b), (top_a, top - top_a, *split3(low))


def source_rows(v):
    (a, b, c), (pa, pb, pc, pd, pe) = squares(v)
    one = jnp.ones_like(v)
    return [a, one, one, pa, pb, a, b, b, a, c, one, one, one, pc, pd, pe]


def target_rows(v, extra):
    (a, b, c), (pa, pb, pc, pd, pe) = squares(v, extra)
    one = jnp.ones_like(v)
    return [-2.0 * a, pa, pb, one, one, -2.0 * b, -2.0 * a, -2.0 * b, -2.0 * c, -2.0 * a, pc, pd, pe, one, one, one]


def stage_sources(ref, i, rows, base):
    at = pl.ds(pl.multiple_of(i * 8, 8), 8)
    pieces = []
    mass = ref[3, at, :] * (1.0 / (cut_sq * cut_sq))
    sums = list(split3(mass))
    for d in range(3):
        place = ref[d, at, :] - 0.5
        pieces += source_rows(place)
        sums += list(split3(mass * place))
    for k, piece in enumerate(pieces + sums):
        rows[base + k * 8:base + k * 8 + 8, :] = piece


def staged(rows, base, j, first, count):
    return rows[pl.ds(base + first * 8 + j, count, stride=8), :]


def stage_targets(own_ref, rows, right):
    def some(i, _):
        at = pl.ds(pl.multiple_of(i * 8, 8), 8)
        for d in range(3):
            base = own_ref[d, at, :] - 0.5
            for o in range(3):
                where = (d * 3 + o) * 128
                for k, piece in enumerate(target_rows(base - float(o - 1), soft_sq if d == 2 else 0.0)):
                    rows[where + k * 8:where + k * 8 + 8, :] = piece
                for j in range(8):
                    right[i * 8 + j, d * 3 + o] = staged(rows, where, j, 0, 16).astype(bf16)
        return 0

    lax.fori_loop(0, own_ref.shape[1] // 8, some, 0)


def weighted(left, right, moments):
    q = jnp.dot(left, right, preferred_element_type=f32)
    r = lax.rsqrt(q)
    t = jnp.maximum((cut_sq + soft_sq) - q, 0.0) * r
    w = t * t * r
    hi = w.astype(bf16)
    lo = (w - hi.astype(f32)).astype(bf16)
    return jnp.dot(
        jnp.concatenate([moments, moments], axis=1), jnp.concatenate([hi, lo], axis=0), preferred_element_type=f32
    )


def paired(count, step):
    def two(i, _):
        step(2 * i, 0)
        step(2 * i + 1, 1)
        return 0

    lax.fori_loop(0, count // 2, two, 0)
    if count % 2:
        step(count - 1, 0)


def pull_kernel(plan, *refs):
    kind, group = plan
    own_ref = refs[1]
    sources = {"own": 0, "caps": 2, "rim": 5}[kind]
    at = 2 + sources
    source_refs = refs[2:at] or refs[1:2]
    before = None
    if kind == "own":
        out_ref, right = refs[at:at + 2]
    else:
        right, before, out_ref = refs[at:at + 3]
        at += 1
    rows, acc, raw, items, copied, *feats = refs[at + 2:]
    fetch = pltpu.make_async_copy(refs[0], items, copied)
    fetch.start()
    columns = own_ref.shape[1] // 2
    count = items.shape[0] // 4

    widest = jnp.zeros((), f32)
    for ref in (own_ref, *(source_refs if kind != "own" else ())):
        widest = jnp.maximum(widest, jnp.max(jnp.abs(ref[0:3] - 0.5)))
    calm = widest < near

    def read(n):
        return items[4 * n], items[4 * n + 1], items[4 * n + 2], items[4 * n + 3]

    @pl.when(calm)
    def _():
        acc[...] = jnp.zeros_like(acc)
        if kind == "own":
            left, sums = feats

            def some(i, lane):
                base = lane * 512
                stage_sources(own_ref, i, rows, base)
                for j in range(8):
                    left[i * 8 + j] = staged(rows, base, j, 0, 48).T.astype(bf16)
                    sums[i * 8 + j] = staged(rows, base, j, 48, 16).astype(bf16)

            paired(own_ref.shape[1] // 8, some)
        elif kind == "caps":
            left_caps, sums_caps = feats

            def some(i, lane):
                bases = [lane * 1024, lane * 1024 + 512]
                for ref, base in zip(source_refs, bases):
                    stage_sources(ref, i, rows, base)
                for j in range(8):
                    both = [staged(rows, base, j, 0, 48) for base in bases]
                    left_caps[i * 8 + j] = jnp.concatenate(both, axis=0).T.astype(bf16)
                    both = [staged(rows, base, j, 48, 16) for base in bases]
                    sums_caps[i * 8 + j] = jnp.concatenate(both, axis=0).astype(bf16)

            paired(source_refs[0].shape[1] // 8, some)
        else:
            left, sums, left_caps, sums_caps = feats
            base = 0
            for ref in source_refs:

                def some(i, lane, ref=ref, base=base):
                    where = lane * 512
                    stage_sources(ref, i, rows, where)
                    for c in range(2):
                        column = base + i * 2 + c
                        for z in range(2):
                            left[column * 2 + z] = staged(rows, where, 4 * c + 1 + z, 0, 48).T.astype(bf16)
                            sums[column * 2 + z] = staged(rows, where, 4 * c + 1 + z, 48, 16).astype(bf16)
                        both = [staged(rows, where, 4 * c + 3 * side, 0, 48) for side in range(2)]
                        left_caps[column] = jnp.concatenate(both, axis=0).T.astype(bf16)
                        both = [staged(rows, where, 4 * c + 3 * side, 48, 16) for side in range(2)]
                        sums_caps[column] = jnp.concatenate(both, axis=0).astype(bf16)

                paired(ref.shape[1] // 8, some)
                base += ref.shape[1] // 4
        if kind == "own":
            stage_targets(own_ref, rows, right)
        fetch.wait()

        def some_items(g, _):
            for k in range(group):
                column, source, ox, oy = read(g * group + k)
                me = jnp.minimum(column, columns - 1) * 2
                side = [[jnp.concatenate([right[me + t, ox], right[me + t, 3 + oy], right[me + t, 6 + oz]], axis=0)
                         for oz in range(3)] for t in range(2)]
                got = None
                zed = None
                if kind != "caps":
                    low = weighted(left[source * 2], jnp.concatenate([side[0][1], side[1][0]], axis=1), sums[source * 2])
                    high = weighted(left[source * 2 + 1], jnp.concatenate([side[0][2], side[1][1]], axis=1), sums[source * 2 + 1])
                    got = low + high
                    zed = jnp.concatenate([high[:8, :128], -low[:8, 128:]], axis=1)
                if kind != "own":
                    blank = jnp.zeros_like(side[0][0])
                    right_caps = jnp.concatenate(
                        [jnp.concatenate([side[0][0], blank], axis=1), jnp.concatenate([blank, side[1][2]], axis=1)], axis=0
                    )
                    caps = weighted(left_caps[source], right_caps, sums_caps[source])
                    caps_got = jnp.concatenate([caps[:16, :128], caps[16:, 128:]], axis=1)
                    caps_zed = jnp.concatenate([-caps[:8, :128], caps[16:24, 128:]], axis=1)
                    got = caps_got if got is None else got + caps_got
                    zed = caps_zed if zed is None else zed + caps_zed
                head = got[:8]
                for t in range(2):
                    lanes = slice(128 * t, 128 * t + 128)
                    first = pl.multiple_of((t * (columns + 1) + column) * 40, 8)
                    acc[pl.ds(first, 16), :] += got[:, lanes]
                    acc[pl.ds(first + 16, 8), :] += (ox - 1).astype(f32) * head[:, lanes]
                    acc[pl.ds(first + 24, 8), :] += (oy - 1).astype(f32) * head[:, lanes]
                    acc[pl.ds(first + 32, 8), :] += zed[:, lanes]
            return 0

        lax.fori_loop(0, count // group, some_items, 0)

        def finish(i, _):
            for t in range(2):
                def row(r):
                    return acc[pl.ds((t * (columns + 1) + i * 8) * 40 + r, 8, stride=40), :]

                spot = pl.ds(i * 16 + t, 8, stride=2)
                total = row(0) + row(1) + row(2)
                for d in range(3):
                    moment = row(3 * d + 3) + row(3 * d + 4) + row(3 * d + 5)
                    moment = moment + (row(16 + 8 * d) + row(17 + 8 * d) + row(18 + 8 * d))
                    value = moment - (own_ref[d, spot, :] - 0.5) * total
                    if before is not None:
                        value = value + before[d, spot, :]
                    out_ref[d, spot, :] = value
            return 0

        lax.fori_loop(0, columns // 8, finish, 0)

    @pl.when(jnp.logical_not(calm))
    def _():
        fetch.wait()
        raw[...] = jnp.zeros_like(raw)
        base = 0
        for ref in source_refs:

            def keep(cell, _, ref=ref, base=base):
                for d in range(4):
                    raw[base + cell, d:d + 1, :] = ref[d, pl.ds(cell, 1), :]
                return 0

            lax.fori_loop(0, ref.shape[1], keep, 0)
            base += ref.shape[1]
        out_ref[...] = before[...] if before is not None else jnp.zeros_like(out_ref)
        layers = {"own": (1, 2), "caps": (0, 3), "rim": (0, 1, 2, 3)}[kind]

        def one(n, _):
            column, source, ox, oy = read(n)

            @pl.when(column < columns)
            def _():
                for layer in layers:
                    cell = {"own": source * 2 + layer - 1, "caps": source + (layer // 3) * columns, "rim": source * 4 + layer}[kind]
                    lined = raw[cell].T
                    for t in range(2):
                        if abs(layer - 1 - t) > 1:
                            continue
                        spot = pl.ds(column * 2 + t, 1)
                        offset = ((ox - 1).astype(f32), (oy - 1).astype(f32), float(layer - 1 - t))
                        away = [(lined[:, d:d + 1] + offset[d]) - own_ref[d, spot, :] for d in range(3)]
                        q = away[0] * away[0] + away[1] * away[1] + away[2] * away[2]
                        r = lax.rsqrt(q + soft_sq)
                        taper = jnp.maximum(1.0 - q * (1.0 / cut_sq), 0.0)
                        w = lined[:, 3:4] * (r * r * r) * (taper * taper)
                        for d in range(3):
                            out_ref[d, spot, :] += jnp.sum(w * away[d], axis=0, keepdims=True)
            return 0

        lax.fori_loop(0, count, one, 0)


def listed(grid, kind):
    nx, ny = grid
    found = []
    for tx in range(nx):
        for ty in range(ny):
            for ox in range(3):
                for oy in range(3):
                    x, y = tx + ox - 1, ty + oy - 1
                    inside = 0 <= x < nx and 0 <= y < ny
                    if inside and kind != "rim":
                        found.append((tx * ny + ty, x * ny + y, ox, oy))
                    elif not inside and kind == "rim":
                        beyond = int(x >= nx)
                        if 0 <= x < nx:
                            source = x if y < 0 else nx + x
                        elif 0 <= y < ny:
                            source = 2 * nx + beyond * ny + y
                        else:
                            source = 2 * nx + 2 * ny + 2 * int(y >= ny) + beyond
                        found.append((tx * ny + ty, source, ox, oy))
    return found


def table_of(kind, group, grid):
    items = listed(grid, kind)
    while len(items) % group:
        items.append((grid[0] * grid[1], 0, 1, 1))
    return np.asarray(items, np.int32).reshape(-1)


def pull(kind, group, table, grid, own, source_arrays=(), right=None, before=None):
    nx, ny = grid
    columns = nx * ny
    cells = sum(a.shape[1] for a in source_arrays) if source_arrays else own.shape[1]
    middle = {"own": cells, "caps": 0, "rim": cells // 2}[kind]
    capped = {"own": 0, "caps": cells // 2, "rim": cells // 4}[kind]
    feats = []
    if middle:
        feats += [pltpu.VMEM((middle, 128, 48), bf16), pltpu.VMEM((middle, 16, 128), bf16)]
    if capped:
        feats += [pltpu.VMEM((capped, 128, 96), bf16), pltpu.VMEM((capped, 32, 128), bf16)]
    args = [own, *source_arrays] + ([right, before] if source_arrays else [])
    out = jax.ShapeDtypeStruct((3, own.shape[1], 128), f32)
    made = jax.ShapeDtypeStruct((own.shape[1], 9, 16, 128), bf16)
    in_vmem = pl.BlockSpec(memory_space=pltpu.VMEM)
    pairs = table.size // 4 * (3 if kind == "rim" else 2 if kind == "own" else 1) * 128 * 256
    return pl.pallas_call(
        functools.partial(pull_kernel, (kind, group)),
        out_shape=out if source_arrays else (out, made),
        in_specs=[pl.BlockSpec(memory_space=pltpu.HBM)] + [in_vmem] * len(args),
        out_specs=in_vmem if source_arrays else (in_vmem, in_vmem),
        scratch_shapes=[
            pltpu.VMEM((2048, 128), f32),
            pltpu.VMEM((2 * (columns + 1) * 40, 128), f32),
            pltpu.VMEM((cells, 8, 128), f32),
            pltpu.SMEM(table.shape, jnp.int32),
            pltpu.SemaphoreType.DMA,
            *feats,
        ],
        compiler_params=pltpu.CompilerParams(vmem_limit_bytes=40 * 2**20),
        cost_estimate=pl.CostEstimate(flops=pairs * 40, bytes_accessed=2**20, transcendentals=pairs),
        name="pull_" + kind,
    )(table, *args)


def rolled(axes, step, cells):
    counts = [lax.axis_size(axis) for axis in axes]
    spots = list(np.ndindex(*counts))
    perm = []
    for spot in spots:
        goal = tuple((i + d) % n for i, d, n in zip(spot, step, counts))
        perm.append((spots.index(spot), spots.index(goal)))
    return lax.ppermute(cells, axes, perm)


def rolled_x(cells, axes=("gx",), step=()):
    if lax.axis_size("gx") == 2:
        return rolled(axes, (1, *step), cells)
    return jnp.concatenate([rolled(axes, (1, *step), cells[:, :1]), rolled(axes, (-1, *step), cells[:, 1:])], axis=1)


groups = {"own": 44, "caps": 110, "rim": 34}


def pull_field(own, tables):
    grid = own.shape[1:3]
    slots = own.shape[-1]

    def lined(cells):
        return cells.reshape(4, -1, slots)

    lower = rolled(("gz",), (1,), own[:, :, :, -1:])
    upper = rolled(("gz",), (-1,), own[:, :, :, :1])
    total, right = pull("own", groups["own"], tables["own"], grid, lined(own))
    lower, upper, total = lax.optimization_barrier((lower, upper, total))

    def tall(*where):
        where = (slice(None), *where)
        return jnp.concatenate([lower[where], own[where], upper[where]], axis=3)

    every, first, last = slice(None), slice(0, 1), slice(-1, None)
    front = rolled(("gy",), (1,), tall(every, last))
    back = rolled(("gy",), (-1,), tall(every, first))
    sides = rolled_x(jnp.concatenate([tall(last), tall(first)], axis=1))
    corners = [
        rolled_x(jnp.concatenate([tall(last, row), tall(first, row)], axis=1), ("gx", "gy"), (step,))
        for step, row in ((1, last), (-1, first))
    ]
    total = pull("caps", groups["caps"], tables["caps"], grid, lined(own), [lined(lower), lined(upper)], right, total)
    rim = (front, back, sides, *corners)
    rim, total = lax.optimization_barrier((rim, total))
    total = pull("rim", groups["rim"], tables["rim"], grid, lined(own), [lined(cells) for cells in rim], right, total)
    return total.reshape(3, *own.shape[1:])


def body(halo_position, halo_velocity, halo_mass, cell_counts):
    occupied = lax.broadcasted_iota(jnp.int32, halo_mass.shape, 3) < cell_counts[..., None]
    tables = {kind: jnp.asarray(table_of(kind, group, halo_mass.shape[:2])) for kind, group in groups.items()}
    fields = jnp.concatenate([halo_position, halo_mass[None]], axis=0)
    held = occupied[None] | (lax.broadcasted_iota(jnp.int32, fields.shape, 0) < 3)
    own, tables = lax.optimization_barrier((jnp.where(held, fields, 0.0), tables))
    first_pull = pull_field(own, tables)
    drifted = jnp.where(occupied[None], halo_position + halo_velocity + 0.5 * first_pull, 0.0)
    own = lax.optimization_barrier(jnp.concatenate([drifted, own[3:]], axis=0))
    second_pull = pull_field(own, tables)
    predicted = halo_position + halo_velocity + first_pull / 3.0 + second_pull / 6.0
    return jnp.where(occupied[None], predicted, 0.0)


def solution(mesh):
    return jax.shard_map(
        body,
        mesh=mesh,
        in_specs=(
            P(None, "gx", "gy", "gz", None),
            P(None, "gx", "gy", "gz", None),
            P("gx", "gy", "gz", None),
            P("gx", "gy", "gz"),
        ),
        out_specs=P(None, "gx", "gy", "gz", None),
        check_vma=False,
    )
```

```python
import functools
import jax
import jax.numpy as jnp
import numpy as np
from jax import lax
from jax.experimental import pallas as pl
from jax.experimental.pallas import tpu as pltpu
from jax.sharding import PartitionSpec as P

soft_sq = 0.01
cut_sq = 0.64
near = 6.0
f32, bf16 = jnp.float32, jnp.bfloat16


def rounded(v):
    return v.astype(bf16).astype(f32)


def split3(v):
    a = rounded(v)
    rest = v - a
    b = rounded(rest)
    return a, b, rest - b


def squares(v, extra=0.0):
    a = rounded(v)
    rest = v - a
    b = rounded(rest)
    top = a * a
    top_a = rounded(top)
    low = 2.0 * a * rest + rest * rest + extra
    return (a, b, rest - b), (top_a, top - top_a, *split3(low))


def source_rows(v):
    (a, b, c), (pa, pb, pc, pd, pe) = squares(v)
    one = jnp.ones_like(v)
    return [a, one, one, pa, pb, a, b, b, a, c, one, one, one, pc, pd, pe]


def target_rows(v, extra):
    (a, b, c), (pa, pb, pc, pd, pe) = squares(v, extra)
    one = jnp.ones_like(v)
    return [-2.0 * a, pa, pb, one, one, -2.0 * b, -2.0 * a, -2.0 * b, -2.0 * c, -2.0 * a, pc, pd, pe, one, one, one]


def stage_sources(ref, i, rows, base):
    at = pl.ds(pl.multiple_of(i * 8, 8), 8)
    pieces = []
    mass = ref[3, at, :] * (1.0 / (cut_sq * cut_sq))
    sums = list(split3(mass))
    for d in range(3):
        place = ref[d, at, :] - 0.5
        pieces += source_rows(place)
        sums += list(split3(mass * place))
    for k, piece in enumerate(pieces + sums):
        rows[base + k * 8:base + k * 8 + 8, :] = piece


def staged(rows, base, j, first, count):
    return rows[pl.ds(base + first * 8 + j, count, stride=8), :]


def stage_targets(own_ref, rows, right):
    def some(i, _):
        at = pl.ds(pl.multiple_of(i * 8, 8), 8)
        for d in range(3):
            base = own_ref[d, at, :] - 0.5
            for o in range(3):
                where = (d * 3 + o) * 128
                for k, piece in enumerate(target_rows(base - float(o - 1), soft_sq if d == 2 else 0.0)):
                    rows[where + k * 8:where + k * 8 + 8, :] = piece
                for j in range(8):
                    right[i * 8 + j, d * 3 + o] = staged(rows, where, j, 0, 16).astype(bf16)
        return 0

    lax.fori_loop(0, own_ref.shape[1] // 8, some, 0)


def weighted(left, right, moments):
    q = jnp.dot(left, right, preferred_element_type=f32)
    r = lax.rsqrt(q)
    t = jnp.maximum((cut_sq + soft_sq) - q, 0.0) * r
    w = t * t * r
    hi = w.astype(bf16)
    lo = (w - hi.astype(f32)).astype(bf16)
    return jnp.dot(
        jnp.concatenate([moments, moments], axis=1), jnp.concatenate([hi, lo], axis=0), preferred_element_type=f32
    )


def paired(count, step):
    def two(i, _):
        step(2 * i, 0)
        step(2 * i + 1, 1)
        return 0

    lax.fori_loop(0, count // 2, two, 0)
    if count % 2:
        step(count - 1, 0)


def pull_kernel(plan, *refs):
    kind, group = plan
    own_ref = refs[1]
    sources = {"own": 0, "caps": 2, "rim": 5}[kind]
    at = 2 + sources
    source_refs = refs[2:at] or refs[1:2]
    before = None
    if kind == "own":
        out_ref, right = refs[at:at + 2]
    else:
        right, before, out_ref = refs[at:at + 3]
        at += 1
    rows, acc, raw, items, copied, *feats = refs[at + 2:]
    fetch = pltpu.make_async_copy(refs[0], items, copied)
    fetch.start()
    columns = own_ref.shape[1] // 2
    count = items.shape[0] // 4

    widest = jnp.zeros((), f32)
    for ref in (own_ref, *(source_refs if kind != "own" else ())):
        widest = jnp.maximum(widest, jnp.max(jnp.abs(ref[0:3] - 0.5)))
    calm = widest < near

    def read(n):
        return items[4 * n], items[4 * n + 1], items[4 * n + 2], items[4 * n + 3]

    @pl.when(calm)
    def _():
        acc[...] = jnp.zeros_like(acc)
        if kind == "own":
            left, sums = feats

            def some(i, lane):
                base = lane * 512
                stage_sources(own_ref, i, rows, base)
                for j in range(8):
                    left[i * 8 + j] = staged(rows, base, j, 0, 48).T.astype(bf16)
                    sums[i * 8 + j] = staged(rows, base, j, 48, 16).astype(bf16)

            paired(own_ref.shape[1] // 8, some)
        elif kind == "caps":
            left_caps, sums_caps = feats

            def some(i, lane):
                bases = [lane * 1024, lane * 1024 + 512]
                for ref, base in zip(source_refs, bases):
                    stage_sources(ref, i, rows, base)
                for j in range(8):
                    both = [staged(rows, base, j, 0, 48) for base in bases]
                    left_caps[i * 8 + j] = jnp.concatenate(both, axis=0).T.astype(bf16)
                    both = [staged(rows, base, j, 48, 16) for base in bases]
                    sums_caps[i * 8 + j] = jnp.concatenate(both, axis=0).astype(bf16)

            paired(source_refs[0].shape[1] // 8, some)
        else:
            left, sums, left_caps, sums_caps = feats
            base = 0
            for ref in source_refs:

                def some(i, lane, ref=ref, base=base):
                    where = lane * 512
                    stage_sources(ref, i, rows, where)
                    for c in range(2):
                        column = base + i * 2 + c
                        for z in range(2):
                            left[column * 2 + z] = staged(rows, where, 4 * c + 1 + z, 0, 48).T.astype(bf16)
                            sums[column * 2 + z] = staged(rows, where, 4 * c + 1 + z, 48, 16).astype(bf16)
                        both = [staged(rows, where, 4 * c + 3 * side, 0, 48) for side in range(2)]
                        left_caps[column] = jnp.concatenate(both, axis=0).T.astype(bf16)
                        both = [staged(rows, where, 4 * c + 3 * side, 48, 16) for side in range(2)]
                        sums_caps[column] = jnp.concatenate(both, axis=0).astype(bf16)

                paired(ref.shape[1] // 8, some)
                base += ref.shape[1] // 4
        if kind == "own":
            stage_targets(own_ref, rows, right)
        fetch.wait()

        def some_items(g, _):
            for k in range(group):
                column, source, ox, oy = read(g * group + k)
                me = jnp.minimum(column, columns - 1) * 2
                side = [[jnp.concatenate([right[me + t, ox], right[me + t, 3 + oy], right[me + t, 6 + oz]], axis=0)
                         for oz in range(3)] for t in range(2)]
                got = None
                zed = None
                if kind != "caps":
                    low = weighted(left[source * 2], jnp.concatenate([side[0][1], side[1][0]], axis=1), sums[source * 2])
                    high = weighted(left[source * 2 + 1], jnp.concatenate([side[0][2], side[1][1]], axis=1), sums[source * 2 + 1])
                    got = low + high
                    zed = jnp.concatenate([high[:8, :128], -low[:8, 128:]], axis=1)
                if kind != "own":
                    blank = jnp.zeros_like(side[0][0])
                    right_caps = jnp.concatenate(
                        [jnp.concatenate([side[0][0], blank], axis=1), jnp.concatenate([blank, side[1][2]], axis=1)], axis=0
                    )
                    caps = weighted(left_caps[source], right_caps, sums_caps[source])
                    caps_got = jnp.concatenate([caps[:16, :128], caps[16:, 128:]], axis=1)
                    caps_zed = jnp.concatenate([-caps[:8, :128], caps[16:24, 128:]], axis=1)
                    got = caps_got if got is None else got + caps_got
                    zed = caps_zed if zed is None else zed + caps_zed
                head = got[:8]
                for t in range(2):
                    lanes = slice(128 * t, 128 * t + 128)
                    first = pl.multiple_of((t * (columns + 1) + column) * 40, 8)
                    acc[pl.ds(first, 16), :] += got[:, lanes]
                    acc[pl.ds(first + 16, 8), :] += (ox - 1).astype(f32) * head[:, lanes]
                    acc[pl.ds(first + 24, 8), :] += (oy - 1).astype(f32) * head[:, lanes]
                    acc[pl.ds(first + 32, 8), :] += zed[:, lanes]
            return 0

        lax.fori_loop(0, count // group, some_items, 0)

        def finish(i, _):
            for t in range(2):
                def row(r):
                    return acc[pl.ds((t * (columns + 1) + i * 8) * 40 + r, 8, stride=40), :]

                spot = pl.ds(i * 16 + t, 8, stride=2)
                total = row(0) + row(1) + row(2)
                for d in range(3):
                    moment = row(3 * d + 3) + row(3 * d + 4) + row(3 * d + 5)
                    moment = moment + (row(16 + 8 * d) + row(17 + 8 * d) + row(18 + 8 * d))
                    value = moment - (own_ref[d, spot, :] - 0.5) * total
                    if before is not None:
                        value = value + before[d, spot, :]
                    out_ref[d, spot, :] = value
            return 0

        lax.fori_loop(0, columns // 8, finish, 0)

    @pl.when(jnp.logical_not(calm))
    def _():
        fetch.wait()
        raw[...] = jnp.zeros_like(raw)
        base = 0
        for ref in source_refs:

            def keep(cell, _, ref=ref, base=base):
                for d in range(4):
                    raw[base + cell, d:d + 1, :] = ref[d, pl.ds(cell, 1), :]
                return 0

            lax.fori_loop(0, ref.shape[1], keep, 0)
            base += ref.shape[1]
        out_ref[...] = before[...] if before is not None else jnp.zeros_like(out_ref)
        layers = {"own": (1, 2), "caps": (0, 3), "rim": (0, 1, 2, 3)}[kind]

        def one(n, _):
            column, source, ox, oy = read(n)

            @pl.when(column < columns)
            def _():
                for layer in layers:
                    cell = {"own": source * 2 + layer - 1, "caps": source + (layer // 3) * columns, "rim": source * 4 + layer}[kind]
                    lined = raw[cell].T
                    for t in range(2):
                        if abs(layer - 1 - t) > 1:
                            continue
                        spot = pl.ds(column * 2 + t, 1)
                        offset = ((ox - 1).astype(f32), (oy - 1).astype(f32), float(layer - 1 - t))
                        away = [(lined[:, d:d + 1] + offset[d]) - own_ref[d, spot, :] for d in range(3)]
                        q = away[0] * away[0] + away[1] * away[1] + away[2] * away[2]
                        r = lax.rsqrt(q + soft_sq)
                        taper = jnp.maximum(1.0 - q * (1.0 / cut_sq), 0.0)
                        w = lined[:, 3:4] * (r * r * r) * (taper * taper)
                        for d in range(3):
                            out_ref[d, spot, :] += jnp.sum(w * away[d], axis=0, keepdims=True)
            return 0

        lax.fori_loop(0, count, one, 0)


def listed(grid, kind):
    nx, ny = grid
    found = []
    for tx in range(nx):
        for ty in range(ny):
            for ox in range(3):
                for oy in range(3):
                    x, y = tx + ox - 1, ty + oy - 1
                    inside = 0 <= x < nx and 0 <= y < ny
                    if inside and kind != "rim":
                        found.append((tx * ny + ty, x * ny + y, ox, oy))
                    elif not inside and kind == "rim":
                        beyond = int(x >= nx)
                        if 0 <= x < nx:
                            source = x if y < 0 else nx + x
                        elif 0 <= y < ny:
                            source = 2 * nx + beyond * ny + y
                        else:
                            source = 2 * nx + 2 * ny + 2 * int(y >= ny) + beyond
                        found.append((tx * ny + ty, source, ox, oy))
    return found


def table_of(kind, group, grid):
    items = listed(grid, kind)
    while len(items) % group:
        items.append((grid[0] * grid[1], 0, 1, 1))
    return np.asarray(items, np.int32).reshape(-1)


def pull(kind, group, table, grid, own, source_arrays=(), right=None, before=None):
    nx, ny = grid
    columns = nx * ny
    cells = sum(a.shape[1] for a in source_arrays) if source_arrays else own.shape[1]
    middle = {"own": cells, "caps": 0, "rim": cells // 2}[kind]
    capped = {"own": 0, "caps": cells // 2, "rim": cells // 4}[kind]
    feats = []
    if middle:
        feats += [pltpu.VMEM((middle, 128, 48), bf16), pltpu.VMEM((middle, 16, 128), bf16)]
    if capped:
        feats += [pltpu.VMEM((capped, 128, 96), bf16), pltpu.VMEM((capped, 32, 128), bf16)]
    args = [own, *source_arrays] + ([right, before] if source_arrays else [])
    out = jax.ShapeDtypeStruct((3, own.shape[1], 128), f32)
    made = jax.ShapeDtypeStruct((own.shape[1], 9, 16, 128), bf16)
    in_vmem = pl.BlockSpec(memory_space=pltpu.VMEM)
    pairs = table.size // 4 * (3 if kind == "rim" else 2 if kind == "own" else 1) * 128 * 256
    return pl.pallas_call(
        functools.partial(pull_kernel, (kind, group)),
        out_shape=out if source_arrays else (out, made),
        in_specs=[pl.BlockSpec(memory_space=pltpu.HBM)] + [in_vmem] * len(args),
        out_specs=in_vmem if source_arrays else (in_vmem, in_vmem),
        scratch_shapes=[
            pltpu.VMEM((2048, 128), f32),
            pltpu.VMEM((2 * (columns + 1) * 40, 128), f32),
            pltpu.VMEM((cells, 8, 128), f32),
            pltpu.SMEM(table.shape, jnp.int32),
            pltpu.SemaphoreType.DMA,
            *feats,
        ],
        compiler_params=pltpu.CompilerParams(vmem_limit_bytes=40 * 2**20),
        cost_estimate=pl.CostEstimate(flops=pairs * 40, bytes_accessed=2**20, transcendentals=pairs),
        name="pull_" + kind,
    )(table, *args)


def rolled(axes, step, cells):
    counts = [lax.axis_size(axis) for axis in axes]
    spots = list(np.ndindex(*counts))
    perm = []
    for spot in spots:
        goal = tuple((i + d) % n for i, d, n in zip(spot, step, counts))
        perm.append((spots.index(spot), spots.index(goal)))
    return lax.ppermute(cells, axes, perm)


def rolled_x(cells, axes=("gx",), step=()):
    if lax.axis_size("gx") == 2:
        return rolled(axes, (1, *step), cells)
    return jnp.concatenate([rolled(axes, (1, *step), cells[:, :1]), rolled(axes, (-1, *step), cells[:, 1:])], axis=1)


groups = {"own": 55, "caps": 110, "rim": 23}


def pull_field(own, tables):
    grid = own.shape[1:3]
    slots = own.shape[-1]

    def lined(cells):
        return cells.reshape(4, -1, slots)

    lower = rolled(("gz",), (1,), own[:, :, :, -1:])
    upper = rolled(("gz",), (-1,), own[:, :, :, :1])
    total, right = pull("own", groups["own"], tables["own"], grid, lined(own))
    lower, upper, total = lax.optimization_barrier((lower, upper, total))

    def tall(*where):
        where = (slice(None), *where)
        return jnp.concatenate([lower[where], own[where], upper[where]], axis=3)

    every, first, last = slice(None), slice(0, 1), slice(-1, None)
    front = rolled(("gy",), (1,), tall(every, last))
    back = rolled(("gy",), (-1,), tall(every, first))
    sides = rolled_x(jnp.concatenate([tall(last), tall(first)], axis=1))
    corners = [
        rolled_x(jnp.concatenate([tall(last, row), tall(first, row)], axis=1), ("gx", "gy"), (step,))
        for step, row in ((1, last), (-1, first))
    ]
    total = pull("caps", groups["caps"], tables["caps"], grid, lined(own), [lined(lower), lined(upper)], right, total)
    rim = (front, back, sides, *corners)
    rim, total = lax.optimization_barrier((rim, total))
    total = pull("rim", groups["rim"], tables["rim"], grid, lined(own), [lined(cells) for cells in rim], right, total)
    return total.reshape(3, *own.shape[1:])


def body(halo_position, halo_velocity, halo_mass, cell_counts):
    occupied = lax.broadcasted_iota(jnp.int32, halo_mass.shape, 3) < cell_counts[..., None]
    tables = {kind: jnp.asarray(table_of(kind, group, halo_mass.shape[:2])) for kind, group in groups.items()}
    fields = jnp.concatenate([halo_position, halo_mass[None]], axis=0)
    held = occupied[None] | (lax.broadcasted_iota(jnp.int32, fields.shape, 0) < 3)
    own, tables = lax.optimization_barrier((jnp.where(held, fields, 0.0), tables))
    first_pull = pull_field(own, tables)
    drifted = jnp.where(occupied[None], halo_position + halo_velocity + 0.5 * first_pull, 0.0)
    own = lax.optimization_barrier(jnp.concatenate([drifted, own[3:]], axis=0))
    second_pull = pull_field(own, tables)
    predicted = halo_position + halo_velocity + first_pull / 3.0 + second_pull / 6.0
    return jnp.where(occupied[None], predicted, 0.0)


def solution(mesh):
    return jax.shard_map(
        body,
        mesh=mesh,
        in_specs=(
            P(None, "gx", "gy", "gz", None),
            P(None, "gx", "gy", "gz", None),
            P("gx", "gy", "gz", None),
            P("gx", "gy", "gz"),
        ),
        out_specs=P(None, "gx", "gy", "gz", None),
        check_vma=False,
    )
```
